32 devices in a mesh: pi: 4 (over y, x), pj: 8 (over z, core).
Axes of the slice: x: 2, y: 2, z: 4, core: 2. Of those that a mesh axis runs over, the one named last changes fastest.
Arguments:
- duo_embedding: bfloat16 [1024, 1024, 128], P('pi', 'pj'), may hold values from -12 to 12
- duo_attention_weights: float32 [128, 8], replicated, may hold values from -16 to 16
- aligned_embedding: bfloat16 [256, 64, 1024], P('pj', None, 'pi'), may hold values from -6 to 6
- aligned_scaling_weights: float32 [64], replicated, may hold values from 0.5 to 1.5
- aligned_shift_vector: float32 [64], replicated, may hold values from -3 to 3
- payload_weights: bfloat16 [64, 256], replicated, may hold values from -0.75 to 0.75
- switch_weights: bfloat16 [64, 256], replicated, may hold values from -0.75 to 0.75
- closing_weights: bfloat16 [256, 64], replicated, may hold values from -1.5 to 1.5
Outputs:
- update: bfloat16 [256, 64, 1024], P('pj', None, 'pi')
The draws below stay inside these ranges and needn't reach their ends.
All inputs are finite; a program needn't handle non-finite values.
Results may differ from the reference program's by a relative error of at most 0.009.
Values may be sent and summed in bfloat16 or wider, within the bound.
A program may use at most 192 MiB of HBM per device.

```python
import math
import jax
import jax.numpy as jnp
from jax import lax

ALIGNED_EMBED = 64
CZ = 128
ATTENDER_TALLY = 8
UNIT_SPAN = 32
POSITION_TALLY = 1024
ALIGNED_SEQS = 256
JOINT_SPAN = 256


def head_directions(key):
    random_dirs = jax.random.normal(jax.random.fold_in(key, 7001), (ATTENDER_TALLY, CZ), jnp.float32)
    random_dirs = random_dirs - jnp.mean(random_dirs, axis=1, keepdims=True)
    return random_dirs / jnp.sqrt(jnp.sum(random_dirs * random_dirs, axis=1, keepdims=True))


def score_weights(key):
    directions = head_directions(key)
    noise = jnp.clip(jax.random.normal(jax.random.fold_in(key, 7002), (CZ, ATTENDER_TALLY), jnp.float32), -6.0, 6.0)
    return 0.18 * noise + 0.35 * directions.T


def draw_duo_attention_weights(key, part):
    return score_weights(key)


def draw_duo_embedding(key, part):
    directions = head_directions(key)
    noise = jnp.clip(jax.random.normal(jax.random.fold_in(key, 7003), (POSITION_TALLY, POSITION_TALLY, CZ), jnp.float32), -6.0, 6.0)
    column_ramp = 2.0 * (2.0 * jnp.arange(POSITION_TALLY, dtype=jnp.float32) / (POSITION_TALLY - 1) - 1.0)
    pair_field = noise + column_ramp[None, :, None] * jnp.sum(directions, axis=0)[None, None, :]
    return pair_field.astype(jnp.bfloat16)


def level_of(key, extent, shards, least, high):
    loudness = 1.0
    for position, blocks in shards:
        heights = jax.random.uniform(jax.random.fold_in(jax.random.fold_in(key, 6), position), (blocks,), jnp.float32, least / len(shards), high / len(shards))
        loudness = loudness * jnp.repeat(jnp.exp(heights), extent[position] // blocks).reshape((-1,) + (1,) * (len(extent) - 1 - position))
    return loudness


def scatter_about(stream_key, extent, width, reach, cuts=(), kind=jnp.bfloat16):
    factor_of = level_of(stream_key, extent, cuts, -0.22, 0.18) if cuts else 1.0
    array = jax.random.normal(stream_key, extent, jnp.float32) * width * factor_of
    return jnp.minimum(jnp.maximum(array, -reach), reach).astype(kind)


def setup_inputs(seed: int = 0) -> dict:
    streams_of = jax.random.split(jax.random.key(seed), 9)
    return {
        "duo_embedding": draw_duo_embedding(jax.random.fold_in(streams_of[8], 71), 0),
        "duo_attention_weights": draw_duo_attention_weights(jax.random.fold_in(streams_of[8], 71), 0),
        "aligned_embedding": scatter_about(streams_of[2], (ALIGNED_SEQS, ALIGNED_EMBED, POSITION_TALLY), 1.0, 6.0, ((0, 8), (2, 4))),
        "aligned_scaling_weights": jnp.clip(1.0 + 0.1 * jax.random.normal(streams_of[3], (ALIGNED_EMBED,), jnp.float32), 0.5, 1.5),
        "aligned_shift_vector": scatter_about(streams_of[4], (ALIGNED_EMBED,), 0.5, 3.0, (), jnp.float32),
        "payload_weights": scatter_about(streams_of[5], (ALIGNED_EMBED, JOINT_SPAN), ALIGNED_EMBED ** -0.5, 0.75),
        "switch_weights": scatter_about(streams_of[6], (ALIGNED_EMBED, JOINT_SPAN), ALIGNED_EMBED ** -0.5, 0.75),
        "closing_weights": scatter_about(streams_of[7], (JOINT_SPAN, ALIGNED_EMBED), (JOINT_SPAN // 16) ** -0.5, 1.5),
    }


EPS = 1e-05

def rescale_embedding(inputs, axis):
    row_mean = lax.optimization_barrier(jnp.mean(inputs, axis=axis, keepdims=True))
    centred = inputs - row_mean
    variance = lax.optimization_barrier(jnp.mean(centred * centred, axis=axis, keepdims=True))
    return centred * lax.rsqrt(variance + EPS)

def reference(duo_embedding, duo_attention_weights, aligned_embedding, aligned_scaling_weights, aligned_shift_vector, payload_weights, switch_weights, closing_weights):
    aligned_fullbit_copy = aligned_embedding.astype(jnp.float32)
    rescaled_aligned = (rescale_embedding(aligned_fullbit_copy, 1) * aligned_scaling_weights[None, :, None] + aligned_shift_vector[None, :, None]).astype(jnp.bfloat16)
    normed_float = rescaled_aligned.astype(jnp.float32)
    payloads = jnp.einsum('scn,ce->sen', normed_float, payload_weights.astype(jnp.float32)).astype(jnp.bfloat16)
    switch_share = jax.nn.sigmoid(jnp.einsum('scn,ce->sen', normed_float, switch_weights.astype(jnp.float32)))
    payload_each_attender = payloads.astype(jnp.float32).reshape(ALIGNED_SEQS, ATTENDER_TALLY, UNIT_SPAN, POSITION_TALLY)
    tile_entries = math.gcd(POSITION_TALLY, 256)
    block_count = POSITION_TALLY // tile_entries

    def one_block(block_index):
        start_position = (block_index * tile_entries).astype(jnp.int32)
        pair_tile = lax.dynamic_slice_in_dim(duo_embedding, start_position, tile_entries, 0).astype(jnp.float32)
        pair_normed = rescale_embedding(pair_tile, 2)
        scores = jnp.einsum('ijc,ch->hij', pair_normed, duo_attention_weights, precision=lax.Precision.HIGHEST)
        row_peak = lax.optimization_barrier(jnp.max(scores, axis=2, keepdims=True))
        exp_scores = jnp.exp(scores - row_peak).astype(jnp.bfloat16)
        exp_float = exp_scores.astype(jnp.float32)
        row_total = lax.optimization_barrier(jnp.sum(exp_float, axis=2))
        numerator = jnp.einsum('hij,shcj->shci', exp_float, payload_each_attender)
        switch_tile = lax.dynamic_slice_in_dim(switch_share, start_position, tile_entries, 2).reshape(ALIGNED_SEQS, ATTENDER_TALLY, UNIT_SPAN, tile_entries)
        averaged_result = (switch_tile * (numerator / row_total[None, :, None, :])).astype(jnp.bfloat16)
        averaged_result = averaged_result.reshape(ALIGNED_SEQS, ATTENDER_TALLY * UNIT_SPAN, tile_entries).astype(jnp.float32)
        return jnp.einsum('ser,ec->scr', averaged_result, closing_weights.astype(jnp.float32)).astype(jnp.bfloat16)
    result_tiles = lax.map(one_block, jnp.arange(block_count, dtype=jnp.int32))
    return jnp.transpose(result_tiles, (1, 2, 0, 3)).reshape(ALIGNED_SEQS, ALIGNED_EMBED, POSITION_TALLY)
```

```python
import functools

import jax
import jax.numpy as jnp
from jax import lax
from jax.experimental import pallas as pl
from jax.experimental.pallas import tpu as pltpu
from jax.sharding import PartitionSpec as P

EPS = 1e-05
MESH = pl.DeviceIdType.MESH
NT = (((1,), (1,)), ((), ()))
CORES = 2
TILE = 16
CHUNK = 32
LAG = 3
GROUP = 8


def dot(a, b, dims=(((1,), (0,)), ((), ()))):
    return lax.dot_general(a, b, dims, preferred_element_type=jnp.float32)


def split_weights(w):
    w = w - jnp.mean(w, axis=1, keepdims=True)
    hi = w.astype(jnp.bfloat16).astype(jnp.float32)
    mid = (w - hi).astype(jnp.bfloat16).astype(jnp.float32)
    w3 = jnp.concatenate([hi, mid, w - hi - mid, jnp.zeros_like(w)], axis=0)
    return w3.astype(jnp.bfloat16)


def tile_scores(x, w3):
    rows, cols, chans = x.shape
    heads = w3.shape[0] // 4
    x = x.reshape(rows * cols, chans)
    mean = dot(x, jnp.ones((chans, chans), jnp.bfloat16)) * (1.0 / chans)
    centred = x.astype(jnp.float32) - mean
    square = centred * centred
    top = square.astype(jnp.bfloat16)
    rest = (square - top.astype(jnp.float32)).astype(jnp.bfloat16)
    ones = jnp.ones((2 * heads, 2 * chans), jnp.bfloat16)
    variance = dot(ones, jnp.concatenate([top, rest], axis=1), NT)[:heads] * (1.0 / chans)
    parts = dot(w3, x, NT)
    scores = parts[:heads] + (parts[heads : 2 * heads] + parts[2 * heads : 3 * heads])
    return scores * lax.rsqrt(variance + EPS)


def kernel(
    pi_count,
    pj_count,
    pair_hbm,
    w_ref,
    msa_hbm,
    gain_ref,
    shift_ref,
    wv_ref,
    ws_ref,
    wc_ref,
    out_ref,
    pair,
    msa,
    ex,
    hold,
    peaks,
    scale,
    vals,
    weights,
    acc,
    gate,
    pair_sem,
    msa_sem,
    ex_rs,
    ex_fw,
    ex_dn,
    ex_pt,
    pk_rs,
    pk_ss,
    ms_rs,
    ms_sx,
    ms_up,
    ms_dn,
):
    me_i, me_j = lax.axis_index("pi"), lax.axis_index("pj")
    line, yline = pj_count // CORES, pi_count // 2
    z, core = me_j // CORES, me_j % CORES
    y, x = me_i // 2, me_i % 2
    chunks = ex.shape[1]
    heads, cols = ex.shape[2], ex.shape[4]
    rows = chunks * CHUNK
    seqs, chans = msa.shape[1], msa.shape[2]
    half = seqs // 2
    span = vals.shape[1] - 16
    width = span // seqs
    mate = me_j - core + (1 - core)
    x_near = me_i - x + (1 - x)

    pair_in = lambda q: pltpu.make_async_copy(
        pair_hbm.at[pl.ds(q * CHUNK, CHUNK)], pair.at[q], pair_sem.at[q]
    )
    own_in = pltpu.make_async_copy(msa_hbm, msa.at[me_i], msa_sem)
    own_in.start()
    lax.fori_loop(0, chunks, lambda q, c: (pair_in(q).start(), c)[1], 0)

    barrier = pltpu.get_barrier_semaphore()

    def greet(i, j):
        pl.semaphore_signal(barrier, inc=1, device_id=(i, j), device_id_type=MESH)

    lax.fori_loop(1, pj_count, lambda r, c: (greet(me_i, (me_j + r) % pj_count), c)[1], 0)
    greet(x_near, me_j)
    up_y, down_y = y < yline - 1, y > 0
    pl.when(up_y)(lambda: greet(me_i + 2, me_j))
    pl.when(down_y)(lambda: greet(me_i - 2, me_j))
    pl.semaphore_wait(barrier, pj_count + jnp.where(up_y, 1, 0) + jnp.where(down_y, 1, 0))

    def part(p, h):
        return msa.at[p, pl.ds(h * half, half)]

    def msa_copy(p, h, send, i):
        return pltpu.make_async_remote_copy(
            part(p, h), part(p, h), send.at[p, h], ms_rs.at[p, h],
            device_id=(i, me_j), device_id_type=MESH,
        )

    def to_x(p, h):
        return msa_copy(p, h, ms_sx, x_near)

    def to_up(p, h):
        return msa_copy(p, h, ms_up, me_i + 2)

    def to_down(p, h):
        return msa_copy(p, h, ms_dn, me_i - 2)

    def along_y(p, h):
        pl.when(up_y)(lambda: to_up(p, h).start())
        pl.when(down_y)(lambda: to_down(p, h).start())

    def take(p, h):
        to_x(p, h).wait_recv()

    own_in.wait()
    to_x(me_i, 0).start()
    along_y(me_i, 1)
    to_x(me_i, 1).start()
    along_y(me_i, 0)

    def pass_y(e, column, h, cross):
        below, above = me_i - x + column - 2 * e, me_i - x + column + 2 * e

        @pl.when(y - e >= 0)
        def _():
            take(below, h)
            pl.when(up_y)(lambda: to_up(below, h).start())
            if cross:
                to_x(below, h).start()

        @pl.when(y + e < yline)
        def _():
            take(above, h)
            pl.when(down_y)(lambda: to_down(above, h).start())
            if cross:
                to_x(above, h).start()

    def first_relays():
        take(x_near, 0)
        along_y(x_near, 0)
        for e in range(1, yline):
            pass_y(e, x, 1, True)

    def ex_copy(o, q, send, j):
        return pltpu.make_async_remote_copy(
            ex.at[o, q], ex.at[o, q], send, ex_rs.at[o, q],
            device_id=(me_i, j), device_id_type=MESH,
        )

    def ex_up(o, q):
        return ex_copy(o, q, ex_fw.at[o, q], me_j + CORES)

    def ex_down(o, q):
        return ex_copy(o, q, ex_fw.at[o, q], me_j - CORES)

    def ex_own_down(q):
        return ex_copy(me_j, q, ex_dn.at[q], me_j - CORES)

    def ex_mate(o, q):
        return ex_copy(o, q, ex_pt.at[o, q], mate)

    up_z, down_z = z < line - 1, z > 0

    def send_own(q):
        pl.when(up_z)(lambda: ex_up(me_j, q).start())
        pl.when(down_z)(lambda: ex_own_down(q).start())
        ex_mate(me_j, q).start()

    def relay(d, q):
        below, above = me_j - CORES * d, me_j + CORES * d

        @pl.when(z - d >= 0)
        def _():
            ex_mate(below, q).wait_recv()
            pl.when(up_z)(lambda: ex_up(below, q).start())
            ex_mate(below, q).start()

        @pl.when(z + d < line)
        def _():
            ex_mate(above, q).wait_recv()
            pl.when(down_z)(lambda: ex_down(above, q).start())
            ex_mate(above, q).start()

    w3 = split_weights(w_ref[...])
    lane = lax.broadcasted_iota(jnp.int32, (heads, rows), 1)
    peaks[me_j] = jnp.zeros((heads, rows), jnp.float32)

    def pair_chunk(q, carry):
        pair_in(q).wait()
        top = peaks[me_j]
        for t in range(CHUNK // TILE):
            scores = tile_scores(pair[q, t * TILE : (t + 1) * TILE], w3)
            for k in range(TILE):
                one = scores[:, k * cols : (k + 1) * cols]
                peak = jnp.max(one, axis=1, keepdims=True)
                hold[:, t * TILE + k, :] = jnp.exp(one - peak)
                top = jnp.where(lane == q * CHUNK + t * TILE + k, peak, top)
        peaks[me_j] = top
        ex[me_j, q] = hold[...].astype(jnp.bfloat16)
        send_own(q)
        pl.when(q >= LAG)(lambda: relay(1, q - LAG))
        pl.when(q == chunks - 1)(first_relays)
        return carry

    lax.fori_loop(0, chunks, pair_chunk, 0)

    def peak_copy(o, j):
        return pltpu.make_async_remote_copy(
            peaks.at[o], peaks.at[o], pk_ss.at[j], pk_rs.at[o],
            device_id=(me_i, j), device_id_type=MESH,
        )

    def others(f):
        lax.fori_loop(1, pj_count, lambda r, c: (f((me_j + r) % pj_count), c)[1], 0)

    others(lambda j: peak_copy(me_j, j).start())

    gain = jnp.broadcast_to(gain_ref[...], (chans, 128))
    shift = jnp.broadcast_to(shift_ref[...], (chans, 128))
    gain = jnp.concatenate([gain] * (rows // 128), axis=1)
    shift = jnp.concatenate([shift] * (rows // 128), axis=1)

    def normed(p, s):
        v = msa[p, s].astype(jnp.float32)
        v = v - jnp.mean(v, axis=0, keepdims=True)
        variance = jnp.mean(v * v, axis=0, keepdims=True)
        return (v * lax.rsqrt(variance + EPS) * gain + shift).astype(jnp.bfloat16)

    def gate_group(g, carry):
        for k in range(GROUP):
            s = g * GROUP + k
            gate[s] = jax.nn.sigmoid(dot(ws_ref[...], normed(me_i, s)))
        return carry

    lax.fori_loop(0, seqs // GROUP, gate_group, 0)

    vals[:, span:, :] = jnp.ones((heads, 16, rows), jnp.bfloat16)

    def zero_head(h, carry):
        acc[h] = jnp.zeros(acc.shape[1:], jnp.float32)
        return carry

    lax.fori_loop(0, heads, zero_head, 0)

    others(lambda j: peak_copy(j, me_j).wait_recv())
    scale[...] = jnp.exp(peaks[...] - jnp.max(peaks[...], axis=0, keepdims=True))

    def process(p):
        pl.when(p % 2 != x)(lambda: take(p, 1))

        def value_group(g, carry):
            for k in range(GROUP):
                s = g * GROUP + k
                v = dot(wv_ref[...], normed(p, s)).astype(jnp.bfloat16)
                at = pl.ds(pl.multiple_of(s * width, width), width)
                for h in range(heads):
                    vals[h, at, :] = v[h * width : (h + 1) * width]
            return carry

        lax.fori_loop(0, seqs // GROUP, value_group, 0)

        far = p * CORES + (1 - core)
        lax.fori_loop(0, chunks, lambda q, c: (ex_mate(far, q).wait_recv(), c)[1], 0)
        both = scale[pl.ds(p * CORES, CORES)].reshape(CORES * heads, rows)
        pad = jnp.zeros((128 - CORES * heads, rows), jnp.float32)
        turned = jnp.concatenate([both, pad], axis=0).T
        for c in range(CORES):
            for h in range(heads):
                e = ex[p * CORES + c, :, h].reshape(rows, cols).astype(jnp.float32)
                e = e * turned[:, c * heads + h : c * heads + h + 1]
                weights[h, :, c * cols : (c + 1) * cols] = e.astype(jnp.bfloat16)

        def head(h, carry):
            acc[h] += dot(vals[h], weights[h], NT)
            return carry

        lax.fori_loop(0, heads, head, 0)

    def stage_of(p):
        apart = jnp.where(p > z, p - z, z - p)
        same_row, same_column = p // 2 == y, p % 2 == x
        kind = jnp.where(same_row | same_column, min(2, line - 1), line - 1)
        kind = jnp.where(p == me_i, 1, kind)
        return jnp.where(apart > kind, apart, kind)

    def stage(d, carry):
        first = jnp.where(d == 1, chunks - LAG, 0)
        lax.fori_loop(first, chunks, lambda q, c: (relay(d, q), c)[1], 0)

        @pl.when(d == min(2, line - 1))
        def _():
            for e in range(1, yline):
                pass_y(e, x, 0, False)

        @pl.when(d == line - 1)
        def _():
            for e in range(1, yline):
                pass_y(e, 1 - x, 0, False)

        def block(p, c):
            pl.when(stage_of(p) == d)(lambda: process(p))
            return c

        lax.fori_loop(0, pi_count, block, 0)
        return carry

    lax.fori_loop(1, line, stage, 0)

    inverse = 1.0 / acc[:, span : span + 8, :]
    inverse = inverse[:, :1, :]

    def close_group(g, carry):
        for k in range(GROUP):
            s = g * GROUP + k
            at = pl.ds(pl.multiple_of(s * width, width), width)
            share = gate[s].reshape(heads, width, rows)
            mixed = (share * (acc[:, at, :] * inverse)).astype(jnp.bfloat16)
            out_ref[s] = dot(wc_ref[...], mixed.reshape(heads * width, rows)).astype(jnp.bfloat16)
        return carry

    lax.fori_loop(0, seqs // GROUP, close_group, 0)

    others(lambda j: peak_copy(me_j, j).wait_send())
    for h in range(2):
        to_x(me_i, h).wait_send()
        for p in (me_i, x_near):
            if h == 0:
                pl.when(up_y)(lambda: to_up(p, h).wait_send())
                pl.when(down_y)(lambda: to_down(p, h).wait_send())
    pl.when(up_y)(lambda: to_up(me_i, 1).wait_send())
    pl.when(down_y)(lambda: to_down(me_i, 1).wait_send())
    for e in range(1, yline):
        for column, h, cross in ((x, 1, True), (x, 0, False), (1 - x, 0, False)):
            below, above = me_i - x + column - 2 * e, me_i - x + column + 2 * e

            @pl.when(y - e >= 0)
            def _():
                pl.when(up_y)(lambda: to_up(below, h).wait_send())
                if cross:
                    to_x(below, h).wait_send()

            @pl.when(y + e < yline)
            def _():
                pl.when(down_y)(lambda: to_down(above, h).wait_send())
                if cross:
                    to_x(above, h).wait_send()

    def drain(q, carry):
        pl.when(up_z)(lambda: ex_up(me_j, q).wait_send())
        pl.when(down_z)(lambda: ex_own_down(q).wait_send())
        ex_mate(me_j, q).wait_send()

        def far_sent(d, c):
            below, above = me_j - CORES * d, me_j + CORES * d

            @pl.when(z - d >= 0)
            def _():
                pl.when(up_z)(lambda: ex_up(below, q).wait_send())
                ex_mate(below, q).wait_send()

            @pl.when(z + d < line)
            def _():
                pl.when(down_z)(lambda: ex_down(above, q).wait_send())
                ex_mate(above, q).wait_send()

            return c

        lax.fori_loop(1, line, far_sent, 0)
        return carry

    lax.fori_loop(0, chunks, drain, 0)


def body(pi_count, pj_count, duo, duo_w, aligned, gain, shift, payload_w, switch_w, closing_w):
    rows, cols, pair_chans = duo.shape
    seqs, chans, tokens = aligned.shape
    heads, joint = duo_w.shape[1], payload_w.shape[1]
    span = seqs * (joint // heads)
    chunks = rows // CHUNK
    assert tokens == rows == CORES * cols and pj_count == CORES * pi_count
    vmem = pl.BlockSpec(memory_space=pltpu.VMEM)
    hbm = pl.BlockSpec(memory_space=pl.ANY)
    dma = pltpu.SemaphoreType.DMA
    return pl.pallas_call(
        functools.partial(kernel, pi_count, pj_count),
        in_specs=[hbm, vmem, hbm] + [vmem] * 5,
        out_specs=vmem,
        out_shape=jax.ShapeDtypeStruct(aligned.shape, jnp.bfloat16),
        scratch_shapes=[
            pltpu.VMEM((chunks, CHUNK, cols, pair_chans), jnp.bfloat16),
            pltpu.VMEM((pi_count, seqs, chans, tokens), jnp.bfloat16),
            pltpu.VMEM((pj_count, chunks, heads, CHUNK, cols), jnp.bfloat16),
            pltpu.VMEM((heads, CHUNK, cols), jnp.float32),
            pltpu.VMEM((pj_count, heads, rows), jnp.float32),
            pltpu.VMEM((pj_count, heads, rows), jnp.float32),
            pltpu.VMEM((heads, span + 16, rows), jnp.bfloat16),
            pltpu.VMEM((heads, rows, CORES * cols), jnp.bfloat16),
            pltpu.VMEM((heads, span + 16, rows), jnp.float32),
            pltpu.VMEM((seqs, joint, tokens), jnp.float32),
            dma((chunks,)),
            dma,
            dma((pj_count, chunks)),
            dma((pj_count, chunks)),
            dma((chunks,)),
            dma((pj_count, chunks)),
            dma((pj_count,)),
            dma((pj_count,)),
            dma((pi_count, 2)),
            dma((pi_count, 2)),
            dma((pi_count, 2)),
            dma((pi_count, 2)),
        ],
        compiler_params=pltpu.CompilerParams(
            collective_id=0, has_side_effects=True, vmem_limit_bytes=60 << 20
        ),
        name="layer",
    )(
        duo,
        duo_w.T,
        aligned,
        gain[:, None],
        shift[:, None],
        payload_w.T,
        switch_w.T,
        closing_w.T,
    )


def solution(mesh):
    return jax.shard_map(
        functools.partial(body, mesh.shape["pi"], mesh.shape["pj"]),
        mesh=mesh,
        in_specs=(P("pi", "pj", None), P(), P("pj", None, "pi"), P(), P(), P(), P(), P()),
        out_specs=P("pj", None, "pi"),
        check_vma=False,
    )
```

```python
import functools

import jax
import jax.numpy as jnp
from jax import lax
from jax.experimental import pallas as pl
from jax.experimental.pallas import tpu as pltpu
from jax.sharding import PartitionSpec as P

EPS = 1e-05
MESH = pl.DeviceIdType.MESH
NT = (((1,), (1,)), ((), ()))
CORES = 2
TILE = 16
CHUNK = 32
GROUP = 8
HELD = 3


def dot(a, b, dims=(((1,), (0,)), ((), ()))):
    return lax.dot_general(a, b, dims, preferred_element_type=jnp.float32)


def split_weights(w):
    w = w - jnp.mean(w, axis=1, keepdims=True)
    hi = w.astype(jnp.bfloat16).astype(jnp.float32)
    mid = (w - hi).astype(jnp.bfloat16).astype(jnp.float32)
    w3 = jnp.concatenate([hi, mid, w - hi - mid, jnp.zeros_like(w)], axis=0)
    return w3.astype(jnp.bfloat16)


def tile_scores(x, w3):
    rows, cols, chans = x.shape
    heads = w3.shape[0] // 4
    x = x.reshape(rows * cols, chans)
    mean = dot(x, jnp.ones((chans, chans), jnp.bfloat16)) * (1.0 / chans)
    centred = x.astype(jnp.float32) - mean
    square = centred * centred
    top = square.astype(jnp.bfloat16)
    rest = (square - top.astype(jnp.float32)).astype(jnp.bfloat16)
    ones = jnp.ones((2 * heads, 2 * chans), jnp.bfloat16)
    variance = dot(ones, jnp.concatenate([top, rest], axis=1), NT)[:heads] * (1.0 / chans)
    parts = dot(w3, x, NT)
    scores = parts[:heads] + (parts[heads : 2 * heads] + parts[2 * heads : 3 * heads])
    return scores * lax.rsqrt(variance + EPS)


def kernel(
    pi_count,
    pj_count,
    pair_hbm,
    w_ref,
    msa_hbm,
    gain_ref,
    shift_ref,
    payload_ref,
    switch_ref,
    wc_ref,
    out_ref,
    wv_ref,
    ws_ref,
    spread,
    pair,
    msa,
    ex,
    hold,
    peaks,
    scale,
    vals,
    weights,
    acc,
    gate,
    pair_sem,
    msa_sem,
    ex_rs,
    ex_fw,
    ex_dn,
    ex_pt,
    pk_rs,
    pk_ss,
    ms_rs,
    ms_sx,
    ms_up,
    ms_dn,
):
    me_i, me_j = lax.axis_index("pi"), lax.axis_index("pj")
    line, yline = pj_count // CORES, pi_count // 2
    z, core = me_j // CORES, me_j % CORES
    y, x = me_i // 2, me_i % 2
    chunks = ex.shape[1]
    heads, cols = ex.shape[2], ex.shape[4]
    rows = chunks * CHUNK
    seqs, chans = msa.shape[1], msa.shape[2]
    half = seqs // 2
    span = vals.shape[2] - 16
    width = span // seqs
    mate = me_j - core + (1 - core)
    x_near = me_i - x + (1 - x)

    pair_in = lambda q: pltpu.make_async_copy(
        pair_hbm.at[pl.ds(q * CHUNK, CHUNK)], pair.at[q], pair_sem.at[q]
    )
    own_in = pltpu.make_async_copy(msa_hbm, msa.at[me_i], msa_sem)
    own_in.start()
    lax.fori_loop(0, chunks, lambda q, c: (pair_in(q).start(), c)[1], 0)

    barrier = pltpu.get_barrier_semaphore()

    def greet(i, j):
        pl.semaphore_signal(barrier, inc=1, device_id=(i, j), device_id_type=MESH)

    lax.fori_loop(1, pj_count, lambda r, c: (greet(me_i, (me_j + r) % pj_count), c)[1], 0)
    greet(x_near, me_j)
    up_y, down_y = y < yline - 1, y > 0
    pl.when(up_y)(lambda: greet(me_i + 2, me_j))
    pl.when(down_y)(lambda: greet(me_i - 2, me_j))

    wv_ref[...] = payload_ref[...].astype(jnp.float32).T.astype(jnp.bfloat16)
    ws_ref[...] = switch_ref[...].astype(jnp.float32).T.astype(jnp.bfloat16)
    diagonal = lax.broadcasted_iota(jnp.int32, (chans, chans), 0)
    diagonal = diagonal == lax.broadcasted_iota(jnp.int32, (chans, chans), 1)
    for k, ref in enumerate((gain_ref, shift_ref)):
        column = jnp.sum(jnp.where(diagonal, ref[...], 0.0), axis=1, keepdims=True)
        spread[k] = jnp.broadcast_to(column, (chans, rows))

    w3 = split_weights(w_ref[...])
    lane = lax.broadcasted_iota(jnp.int32, (heads, rows), 1)
    peaks[me_j] = jnp.zeros((heads, rows), jnp.float32)

    def pair_chunk(q):
        pair_in(q).wait()
        top = peaks[me_j]
        for t in range(CHUNK // TILE):
            scores = tile_scores(pair[q, t * TILE : (t + 1) * TILE], w3)
            for k in range(TILE):
                one = scores[:, k * cols : (k + 1) * cols]
                peak = jnp.max(one, axis=1, keepdims=True)
                hold[:, t * TILE + k, :] = jnp.exp(one - peak)
                top = jnp.where(lane == q * CHUNK + t * TILE + k, peak, top)
        peaks[me_j] = top
        ex[me_j, q] = hold[...].astype(jnp.bfloat16)

    pair_chunk(0)

    pl.semaphore_wait(barrier, pj_count + jnp.where(up_y, 1, 0) + jnp.where(down_y, 1, 0))

    def part(p, h):
        return msa.at[p, pl.ds(h * half, half)]

    def msa_copy(p, h, send, i):
        return pltpu.make_async_remote_copy(
            part(p, h), part(p, h), send.at[p, h], ms_rs.at[p, h],
            device_id=(i, me_j), device_id_type=MESH,
        )

    def to_x(p, h):
        return msa_copy(p, h, ms_sx, x_near)

    def to_up(p, h):
        return msa_copy(p, h, ms_up, me_i + 2)

    def to_down(p, h):
        return msa_copy(p, h, ms_dn, me_i - 2)

    def along_y(p, h):
        pl.when(up_y)(lambda: to_up(p, h).start())
        pl.when(down_y)(lambda: to_down(p, h).start())

    def take(p, h):
        to_x(p, h).wait_recv()

    own_in.wait()
    to_x(me_i, 0).start()
    along_y(me_i, 1)
    to_x(me_i, 1).start()
    along_y(me_i, 0)

    def pass_y(e, column, h, cross):
        below, above = me_i - x + column - 2 * e, me_i - x + column + 2 * e

        @pl.when(y - e >= 0)
        def _():
            take(below, h)
            pl.when(up_y)(lambda: to_up(below, h).start())
            if cross:
                to_x(below, h).start()

        @pl.when(y + e < yline)
        def _():
            take(above, h)
            pl.when(down_y)(lambda: to_down(above, h).start())
            if cross:
                to_x(above, h).start()

    def first_relays():
        take(x_near, 0)
        along_y(x_near, 0)
        for e in range(1, yline):
            pass_y(e, x, 1, True)

    def ex_copy(o, q, send, j):
        return pltpu.make_async_remote_copy(
            ex.at[o, q], ex.at[o, q], send, ex_rs.at[o, q],
            device_id=(me_i, j), device_id_type=MESH,
        )

    def ex_up(o, q):
        return ex_copy(o, q, ex_fw.at[o, q], me_j + CORES)

    def ex_down(o, q):
        return ex_copy(o, q, ex_fw.at[o, q], me_j - CORES)

    def ex_own_down(q):
        return ex_copy(me_j, q, ex_dn.at[q], me_j - CORES)

    def ex_mate(o, q):
        return ex_copy(o, q, ex_pt.at[o, q], mate)

    up_z, down_z = z < line - 1, z > 0

    def send_own(q):
        pl.when(up_z)(lambda: ex_up(me_j, q).start())
        pl.when(down_z)(lambda: ex_own_down(q).start())
        ex_mate(me_j, q).start()

    def relay(d, q):
        below, above = me_j - CORES * d, me_j + CORES * d

        @pl.when(z - d >= 0)
        def _():
            ex_mate(below, q).wait_recv()
            pl.when(up_z)(lambda: ex_up(below, q).start())
            ex_mate(below, q).start()

        @pl.when(z + d < line)
        def _():
            ex_mate(above, q).wait_recv()
            pl.when(down_z)(lambda: ex_down(above, q).start())
            ex_mate(above, q).start()

    def peak_copy(o, j):
        return pltpu.make_async_remote_copy(
            peaks.at[o], peaks.at[o], pk_ss.at[j], pk_rs.at[o],
            device_id=(me_i, j), device_id_type=MESH,
        )

    def others(f):
        lax.fori_loop(1, pj_count, lambda r, c: (f((me_j + r) % pj_count), c)[1], 0)

    send_own(0)
    lax.fori_loop(1, chunks, lambda q, c: (pair_chunk(q), send_own(q), c)[2], 0)
    others(lambda j: peak_copy(me_j, j).start())

    def relays(d, first, last):
        lax.fori_loop(first, last, lambda q, c: (relay(d, q), c)[1], 0)

    def normed(p, s):
        v = msa[p, s].astype(jnp.float32)
        v = v - jnp.mean(v, axis=0, keepdims=True)
        variance = jnp.mean(v * v, axis=0, keepdims=True)
        return (v * lax.rsqrt(variance + EPS) * spread[0] + spread[1]).astype(jnp.bfloat16)

    def gate_group(g, carry):
        for k in range(GROUP):
            s = g * GROUP + k
            gate[s] = jax.nn.sigmoid(dot(ws_ref[...], normed(me_i, s)))
        return carry

    relays(1, 0, chunks - 2)
    lax.fori_loop(0, seqs // GROUP, gate_group, 0)
    relays(1, chunks - 2, chunks)
    first_relays()

    for slot in range(2):
        vals[slot, :, span:, :] = jnp.ones((heads, 16, rows), jnp.bfloat16)

    def zero_head(h, carry):
        acc[h] = jnp.zeros(acc.shape[1:], jnp.float32)
        return carry

    lax.fori_loop(0, heads, zero_head, 0)

    others(lambda j: peak_copy(j, me_j).wait_recv())
    scale[...] = jnp.exp(peaks[...] - jnp.max(peaks[...], axis=0, keepdims=True))

    def values(p, slot):
        pl.when(p % 2 != x)(lambda: take(p, 1))

        def value_group(g, carry):
            for k in range(GROUP):
                s = g * GROUP + k
                v = dot(wv_ref[...], normed(p, s)).astype(jnp.bfloat16)
                at = pl.ds(pl.multiple_of(s * width, width), width)
                for h in range(heads):
                    vals[slot, h, at, :] = v[h * width : (h + 1) * width]
            return carry

        lax.fori_loop(0, seqs // GROUP, value_group, 0)

    def attend(p, slot):
        far = p * CORES + (1 - core)
        lax.fori_loop(0, chunks, lambda q, c: (ex_mate(far, q).wait_recv(), c)[1], 0)
        both = scale[pl.ds(p * CORES, CORES)].reshape(CORES * heads, rows)
        pad = jnp.zeros((128 - CORES * heads, rows), jnp.float32)
        turned = jnp.concatenate([both, pad], axis=0).T
        for h in range(heads):
            for c in range(CORES):
                e = ex[p * CORES + c, :, h].reshape(rows, cols).astype(jnp.float32)
                e = e * turned[:, c * heads + h : c * heads + h + 1]
                weights[h, :, c * cols : (c + 1) * cols] = e.astype(jnp.bfloat16)
        for h in range(heads):
            acc[h] += dot(vals[slot, h], weights[h], NT)

    def apart(p):
        return jnp.where(p > z, p - z, z - p)

    def crosses(p):
        return (p // 2 != y) & (p % 2 != x)

    def attend_unit(p):
        near = jnp.where(apart(p) <= 1, jnp.where(p == me_i, 0, 1), apart(p))
        unit = jnp.where(crosses(p), line - 1, near)
        return jnp.where(apart(p) == line - 1, line, unit)

    def value_unit(p):
        early = jnp.where(crosses(p), line - 1, line - 2)
        return jnp.where(apart(p) == line - 1, early, attend_unit(p))

    half_way = chunks // 2

    def step(n, carry):
        u, p = n // pi_count, n % pi_count
        fresh = p == 0

        @pl.when(fresh & (u == 1))
        def _():
            for e in range(1, yline):
                pass_y(e, x, 0, False)
            relays(2, 0, half_way)

        @pl.when((u == 1) & (p < chunks - half_way))
        def _():
            relay(2, half_way + p)

        @pl.when(fresh & (u >= 3) & (u < line - 1))
        def _():
            relays(u, 0, chunks)

        @pl.when(fresh & (u == line - 1))
        def _():
            relays(line - 1, 0, chunks - HELD)
            for e in range(1, yline):
                pass_y(e, 1 - x, 0, False)

        @pl.when(fresh & (u == line))
        def _():
            relays(line - 1, chunks - HELD, chunks)

        slot = jnp.where(apart(p) == line - 1, 1, 0)
        pl.when(value_unit(p) == u)(lambda: values(p, slot))
        pl.when(attend_unit(p) == u)(lambda: attend(p, slot))
        return carry

    lax.fori_loop(0, (line + 1) * pi_count, step, 0)

    inverse = 1.0 / acc[:, span : span + 8, :]
    inverse = inverse[:, :1, :]

    def close_group(g, carry):
        for k in range(GROUP):
            s = g * GROUP + k
            at = pl.ds(pl.multiple_of(s * width, width), width)
            share = gate[s].reshape(heads, width, rows)
            mixed = (share * (acc[:, at, :] * inverse)).astype(jnp.bfloat16)
            out_ref[s] = dot(wc_ref[...], mixed.reshape(heads * width, rows)).astype(jnp.bfloat16)
        return carry

    lax.fori_loop(0, seqs // GROUP, close_group, 0)

    others(lambda j: peak_copy(me_j, j).wait_send())
    for h in range(2):
        to_x(me_i, h).wait_send()
        for p in (me_i, x_near):
            if h == 0:
                pl.when(up_y)(lambda: to_up(p, h).wait_send())
                pl.when(down_y)(lambda: to_down(p, h).wait_send())
    pl.when(up_y)(lambda: to_up(me_i, 1).wait_send())
    pl.when(down_y)(lambda: to_down(me_i, 1).wait_send())
    for e in range(1, yline):
        for column, h, cross in ((x, 1, True), (x, 0, False), (1 - x, 0, False)):
            below, above = me_i - x + column - 2 * e, me_i - x + column + 2 * e

            @pl.when(y - e >= 0)
            def _():
                pl.when(up_y)(lambda: to_up(below, h).wait_send())
                if cross:
                    to_x(below, h).wait_send()

            @pl.when(y + e < yline)
            def _():
                pl.when(down_y)(lambda: to_down(above, h).wait_send())
                if cross:
                    to_x(above, h).wait_send()

    def drain(q, carry):
        pl.when(up_z)(lambda: ex_up(me_j, q).wait_send())
        pl.when(down_z)(lambda: ex_own_down(q).wait_send())
        ex_mate(me_j, q).wait_send()

        def far_sent(d, c):
            below, above = me_j - CORES * d, me_j + CORES * d

            @pl.when(z - d >= 0)
            def _():
                pl.when(up_z)(lambda: ex_up(below, q).wait_send())
                ex_mate(below, q).wait_send()

            @pl.when(z + d < line)
            def _():
                pl.when(down_z)(lambda: ex_down(above, q).wait_send())
                ex_mate(above, q).wait_send()

            return c

        lax.fori_loop(1, line, far_sent, 0)
        return carry

    lax.fori_loop(0, chunks, drain, 0)


def body(pi_count, pj_count, duo, duo_w, aligned, gain, shift, payload_w, switch_w, closing_w):
    rows, cols, pair_chans = duo.shape
    seqs, chans, tokens = aligned.shape
    heads, joint = duo_w.shape[1], payload_w.shape[1]
    span = seqs * (joint // heads)
    chunks = rows // CHUNK
    assert tokens == rows == CORES * cols and pj_count == CORES * pi_count
    assert pi_count >= 4 and pi_count >= chunks // 2
    vmem = pl.BlockSpec(memory_space=pltpu.VMEM)
    hbm = pl.BlockSpec(memory_space=pl.ANY)
    dma = pltpu.SemaphoreType.DMA
    return pl.pallas_call(
        functools.partial(kernel, pi_count, pj_count),
        in_specs=[hbm, vmem, hbm] + [vmem] * 5,
        out_specs=vmem,
        out_shape=jax.ShapeDtypeStruct(aligned.shape, jnp.bfloat16),
        scratch_shapes=[
            pltpu.VMEM((joint, chans), jnp.bfloat16),
            pltpu.VMEM((joint, chans), jnp.bfloat16),
            pltpu.VMEM((2, chans, rows), jnp.float32),
            pltpu.VMEM((chunks, CHUNK, cols, pair_chans), jnp.bfloat16),
            pltpu.VMEM((pi_count, seqs, chans, tokens), jnp.bfloat16),
            pltpu.VMEM((pj_count, chunks, heads, CHUNK, cols), jnp.bfloat16),
            pltpu.VMEM((heads, CHUNK, cols), jnp.float32),
            pltpu.VMEM((pj_count, heads, rows), jnp.float32),
            pltpu.VMEM((pj_count, heads, rows), jnp.float32),
            pltpu.VMEM((2, heads, span + 16, rows), jnp.bfloat16),
            pltpu.VMEM((heads, rows, CORES * cols), jnp.bfloat16),
            pltpu.VMEM((heads, span + 16, rows), jnp.float32),
            pltpu.VMEM((seqs, joint, tokens), jnp.float32),
            dma((chunks,)),
            dma,
            dma((pj_count, chunks)),
            dma((pj_count, chunks)),
            dma((chunks,)),
            dma((pj_count, chunks)),
            dma((pj_count,)),
            dma((pj_count,)),
            dma((pi_count, 2)),
            dma((pi_count, 2)),
            dma((pi_count, 2)),
            dma((pi_count, 2)),
        ],
        compiler_params=pltpu.CompilerParams(
            collective_id=0, has_side_effects=True, vmem_limit_bytes=58 << 20
        ),
        name="layer",
    )(
        duo,
        duo_w.T,
        aligned,
        gain[None, :],
        shift[None, :],
        payload_w,
        switch_w,
        closing_w.T,
    )


def solution(mesh):
    return jax.shard_map(
        functools.partial(body, mesh.shape["pi"], mesh.shape["pj"]),
        mesh=mesh,
        in_specs=(P("pi", "pj", None), P(), P("pj", None, "pi"), P(), P(), P(), P(), P()),
        out_specs=P("pj", None, "pi"),
        check_vma=False,
    )
```

```python
import functools

import jax
import jax.numpy as jnp
from jax import lax
from jax.experimental import pallas as pl
from jax.experimental.pallas import tpu as pltpu
from jax.sharding import PartitionSpec as P

EPS = 1e-05
MESH = pl.DeviceIdType.MESH
NT = (((1,), (1,)), ((), ()))
CORES = 2
TILE = 16
CHUNK = 32
GROUP = 16
HELD = 3
VMEM_LIMIT = 58 << 20


def dot(a, b, dims=(((1,), (0,)), ((), ()))):
    return lax.dot_general(a, b, dims, preferred_element_type=jnp.float32)


def split_weights(w):
    w = w - jnp.mean(w, axis=1, keepdims=True)
    hi = w.astype(jnp.bfloat16).astype(jnp.float32)
    mid = (w - hi).astype(jnp.bfloat16).astype(jnp.float32)
    w3 = jnp.concatenate([hi, mid, w - hi - mid, jnp.zeros_like(w)], axis=0)
    return w3.astype(jnp.bfloat16)


def tile_scores(x, w3):
    rows, cols, chans = x.shape
    heads = w3.shape[0] // 4
    x = x.reshape(rows * cols, chans)
    mean = dot(x, jnp.ones((chans, chans), jnp.bfloat16)) * (1.0 / chans)
    centred = x.astype(jnp.float32) - mean
    square = centred * centred
    top = square.astype(jnp.bfloat16)
    rest = (square - top.astype(jnp.float32)).astype(jnp.bfloat16)
    ones = jnp.ones((2 * heads, 2 * chans), jnp.bfloat16)
    variance = dot(ones, jnp.concatenate([top, rest], axis=1), NT)[:heads] * (1.0 / chans)
    parts = dot(w3, x, NT)
    scores = parts[:heads] + (parts[heads : 2 * heads] + parts[2 * heads : 3 * heads])
    return scores * lax.rsqrt(variance + EPS)


def kernel(
    pi_count,
    pj_count,
    pair_hbm,
    w_ref,
    msa_hbm,
    gain_ref,
    shift_ref,
    payload_ref,
    switch_ref,
    wc_ref,
    out_ref,
    wv_ref,
    ws_ref,
    spread,
    pair,
    msa,
    ex,
    hold,
    peaks,
    scale,
    vals,
    weights,
    acc,
    gate,
    pair_sem,
    msa_sem,
    ex_rs,
    ex_fw,
    ex_dn,
    ex_pt,
    ex_far,
    pk_rs,
    pk_ss,
    ms_rs,
    ms_sx,
    ms_up,
    ms_dn,
):
    me_i, me_j = lax.axis_index("pi"), lax.axis_index("pj")
    line, yline = pj_count // CORES, pi_count // 2
    z, core = me_j // CORES, me_j % CORES
    y, x = me_i // 2, me_i % 2
    chunks = ex.shape[1]
    heads, cols = ex.shape[2], ex.shape[4]
    rows = chunks * CHUNK
    seqs, half, chans = out_ref.shape[0], msa.shape[1], msa.shape[2]
    span = vals.shape[2] - 16
    width = span // seqs
    mate = me_j - core + (1 - core)
    x_near = me_i - x + (1 - x)

    pair_in = lambda q: pltpu.make_async_copy(
        pair_hbm.at[pl.ds(q * CHUNK, CHUNK)], pair.at[q], pair_sem.at[q]
    )
    own_in = [
        pltpu.make_async_copy(msa_hbm.at[pl.ds(h * half, half)], msa.at[me_i * 2 + h], msa_sem.at[h])
        for h in range(2)
    ]
    for h in range(2):
        own_in[h].start()
    lax.fori_loop(0, chunks, lambda q, c: (pair_in(q).start(), c)[1], 0)

    barrier = pltpu.get_barrier_semaphore()

    def greet(i, j):
        pl.semaphore_signal(barrier, inc=1, device_id=(i, j), device_id_type=MESH)

    lax.fori_loop(1, pj_count, lambda r, c: (greet(me_i, (me_j + r) % pj_count), c)[1], 0)
    greet(x_near, me_j)
    up_y, down_y = y < yline - 1, y > 0
    pl.when(up_y)(lambda: greet(me_i + 2, me_j))
    pl.when(down_y)(lambda: greet(me_i - 2, me_j))

    pl.semaphore_wait(barrier, pj_count + jnp.where(up_y, 1, 0) + jnp.where(down_y, 1, 0))

    def msa_copy(p, h, send, i, count=1):
        part = msa.at[pl.ds(p * 2 + h, count)]
        return pltpu.make_async_remote_copy(
            part, part, send, ms_rs.at[p, h], device_id=(i, me_j), device_id_type=MESH
        )

    def to_x(p, h):
        return msa_copy(p, h, ms_sx, x_near)

    def to_up(p, h, e):
        return msa_copy(p, h, ms_up.at[e], me_i + 2)

    def to_down(p, h, e):
        return msa_copy(p, h, ms_dn.at[e], me_i - 2)

    def along_y(p, h):
        pl.when(up_y)(lambda: to_up(p, h, 0).start())
        pl.when(down_y)(lambda: to_down(p, h, 0).start())

    def take(p, h):
        to_x(p, h).wait_recv()

    for h in range(2):
        own_in[h].wait()
    to_x(me_i, 0).start()
    along_y(me_i, 1)
    to_x(me_i, 1).start()
    along_y(me_i, 0)

    def pass_y(e, column, h, cross):
        below, above = me_i - x + column - 2 * e, me_i - x + column + 2 * e

        @pl.when(y - e >= 0)
        def _():
            take(below, h)
            pl.when(up_y)(lambda: to_up(below, h, e).start())
            if cross:
                to_x(below, h).start()

        @pl.when(y + e < yline)
        def _():
            take(above, h)
            pl.when(down_y)(lambda: to_down(above, h, e).start())
            if cross:
                to_x(above, h).start()

    def first_relays():
        take(x_near, 0)
        along_y(x_near, 0)
        for e in range(1, yline):
            pass_y(e, x, 1, True)

    def ex_copy(o, q, send, receive, j):
        block = ex.at[o] if q is None else ex.at[o, q]
        return pltpu.make_async_remote_copy(
            block, block, send, receive, device_id=(me_i, j), device_id_type=MESH
        )

    def ex_along(o, q, send, j):
        c = o // CORES
        return ex_copy(o, q, send, ex_rs.at[c, 0 if q is None else q], j)

    def ex_up(o, q=None):
        return ex_along(o, q, ex_fw.at[o // CORES], me_j + CORES)

    def ex_down(o, q=None):
        return ex_along(o, q, ex_fw.at[o // CORES], me_j - CORES)

    def ex_own_down(q=None):
        return ex_along(me_j, q, ex_dn, me_j - CORES)

    def ex_mate(o, q=None):
        return ex_copy(o, q, ex_pt.at[o // CORES], ex_far.at[o // CORES], mate)

    up_z, down_z = z < line - 1, z > 0

    def send_own(q):
        pl.when(up_z)(lambda: ex_up(me_j, q).start())
        pl.when(down_z)(lambda: ex_own_down(q).start())
        ex_mate(me_j, q).start()

    def relay(d, q):
        below, above = me_j - CORES * d, me_j + CORES * d

        @pl.when(z - d >= 0)
        def _():
            ex_up(below, q).wait_recv()
            pl.when(up_z)(lambda: ex_up(below, q).start())
            ex_mate(below, q).start()

        @pl.when(z + d < line)
        def _():
            ex_up(above, q).wait_recv()
            pl.when(down_z)(lambda: ex_down(above, q).start())
            ex_mate(above, q).start()

    def peak_copy(o, j):
        return pltpu.make_async_remote_copy(
            peaks.at[o], peaks.at[o], pk_ss, pk_rs,
            device_id=(me_i, j), device_id_type=MESH,
        )

    def all_peaks():
        part = peaks.at[pl.ds(0, pj_count - 1)]
        return pltpu.make_async_remote_copy(
            part, part, pk_ss, pk_rs, device_id=(me_i, mate), device_id_type=MESH
        )

    def others(f):
        lax.fori_loop(1, pj_count, lambda r, c: (f((me_j + r) % pj_count), c)[1], 0)

    w3 = split_weights(w_ref[...])
    lane = lax.broadcasted_iota(jnp.int32, (heads, rows), 1)
    peaks[me_j] = jnp.zeros((heads, rows), jnp.float32)

    def pair_chunk(q):
        pair_in(q).wait()
        top = peaks[me_j]
        for t in range(CHUNK // TILE):
            scores = tile_scores(pair[q, t * TILE : (t + 1) * TILE], w3)
            for k in range(TILE):
                one = scores[:, k * cols : (k + 1) * cols]
                peak = jnp.max(one, axis=1, keepdims=True)
                hold[:, t * TILE + k, :] = jnp.exp(one - peak)
                top = jnp.where(lane == q * CHUNK + t * TILE + k, peak, top)
        peaks[me_j] = top
        ex[me_j, q] = hold[...].astype(jnp.bfloat16)

    lax.fori_loop(0, chunks, lambda q, c: (pair_chunk(q), send_own(q), c)[2], 0)
    others(lambda j: peak_copy(me_j, j).start())

    def relays(d, first, last):
        lax.fori_loop(first, last, lambda q, c: (relay(d, q), c)[1], 0)

    def normed(p, s):
        v = msa[p * 2 + s // half, s % half].astype(jnp.float32)
        v = v - jnp.mean(v, axis=0, keepdims=True)
        variance = jnp.mean(v * v, axis=0, keepdims=True)
        return (v * lax.rsqrt(variance + EPS) * spread[0] + spread[1]).astype(jnp.bfloat16)

    def gate_group(g, carry):
        for k in range(GROUP):
            s = g * GROUP + k
            gate[s] = jax.nn.sigmoid(dot(ws_ref[...], normed(me_i, s)))
        return carry

    wv_ref[...] = payload_ref[...].astype(jnp.float32).T.astype(jnp.bfloat16)
    ws_ref[...] = switch_ref[...].astype(jnp.float32).T.astype(jnp.bfloat16)
    diagonal = lax.broadcasted_iota(jnp.int32, (chans, chans), 0)
    diagonal = diagonal == lax.broadcasted_iota(jnp.int32, (chans, chans), 1)
    for k, ref in enumerate((gain_ref, shift_ref)):
        column = jnp.sum(jnp.where(diagonal, ref[...], 0.0), axis=1, keepdims=True)
        spread[k] = jnp.broadcast_to(column, (chans, rows))

    relays(1, 0, chunks - 2)
    lax.fori_loop(0, seqs // GROUP, gate_group, 0)
    relays(1, chunks - 2, chunks)
    first_relays()

    for slot in range(2):
        vals[slot, :, span:, :] = jnp.ones((heads, 16, rows), jnp.bfloat16)

    def zero_head(h, carry):
        acc[h] = jnp.zeros(acc.shape[1:], jnp.float32)
        return carry

    lax.fori_loop(0, heads, zero_head, 0)

    all_peaks().wait_recv()
    scale[...] = jnp.exp(peaks[...] - jnp.max(peaks[...], axis=0, keepdims=True))

    def values(p, slot):
        pl.when(p % 2 != x)(lambda: take(p, 1))

        def value_group(g, carry):
            for k in range(GROUP):
                s = g * GROUP + k
                v = dot(wv_ref[...], normed(p, s)).astype(jnp.bfloat16)
                at = pl.ds(pl.multiple_of(s * width, width), width)
                for h in range(heads):
                    vals[slot, h, at, :] = v[h * width : (h + 1) * width]
            return carry

        lax.fori_loop(0, seqs // GROUP, value_group, 0)

    def rescale(p, slot):
        ex_mate(p * CORES + (1 - core)).wait_recv()
        both = scale[pl.ds(p * CORES, CORES)].reshape(CORES * heads, rows)
        pad = jnp.zeros((128 - CORES * heads, rows), jnp.float32)
        turned = jnp.concatenate([both, pad], axis=0).T
        for h in range(heads):
            for c in range(CORES):
                e = ex[p * CORES + c, :, h].reshape(rows, cols).astype(jnp.float32)
                e = e * turned[:, c * heads + h : c * heads + h + 1]
                weights[slot, h, :, c * cols : (c + 1) * cols] = e.astype(jnp.bfloat16)

    def attend(slot, weight_slot):
        for h in range(heads):
            acc[h] += dot(vals[slot, h], weights[weight_slot, h], NT)

    def apart(p):
        return jnp.where(p > z, p - z, z - p)

    def crosses(p):
        return (p // 2 != y) & (p % 2 != x)

    def attend_unit(p):
        near = jnp.where(apart(p) <= 1, jnp.where(p == me_i, 0, 1), apart(p))
        unit = jnp.where(crosses(p), line - 1, near)
        return jnp.where(apart(p) == line - 1, line, unit)

    def value_unit(p):
        early = jnp.where(crosses(p), line - 1, line - 2)
        return jnp.where(apart(p) == line - 1, early, attend_unit(p))

    half_way = chunks // 2
    diagonal_block = (y + 1) % yline * 2 + (1 - x)

    def step(n, carry):
        u, p = n // pi_count, n % pi_count
        fresh = p == 0

        @pl.when(fresh & (u == 1))
        def _():
            relays(2, 0, half_way)
            for e in range(1, yline):
                pass_y(e, x, 0, False)

        @pl.when((u == 1) & (p < chunks - half_way))
        def _():
            relay(2, half_way + p)

        @pl.when(fresh & (u >= 3) & (u < line - 1))
        def _():
            relays(u, 0, chunks)

        @pl.when(fresh & (u == line - 1))
        def _():
            relays(line - 1, 0, chunks - HELD)
            for e in range(1, yline):
                pass_y(e, 1 - x, 0, False)

        @pl.when(fresh & (u == line))
        def _():
            relays(line - 1, chunks - HELD, chunks)

        slot = jnp.where(apart(p) == line - 1, 1, 0)
        early = (p == diagonal_block) & (slot == 0)
        weight_slot = jnp.where(early, 2, slot)
        rescale_unit = jnp.where(early, line - 2, attend_unit(p))
        pl.when(value_unit(p) == u)(lambda: values(p, slot))
        pl.when(rescale_unit == u)(lambda: rescale(p, weight_slot))
        pl.when(attend_unit(p) == u)(lambda: attend(slot, weight_slot))
        return carry

    lax.fori_loop(0, (line + 1) * pi_count, step, 0)

    inverse = 1.0 / acc[:, span : span + 8, :]
    inverse = inverse[:, :1, :]

    def close_group(g, carry):
        for k in range(GROUP):
            s = g * GROUP + k
            at = pl.ds(pl.multiple_of(s * width, width), width)
            share = gate[s].reshape(heads, width, rows)
            mixed = (share * (acc[:, at, :] * inverse)).astype(jnp.bfloat16)
            out_ref[s] = dot(wc_ref[...], mixed.reshape(heads * width, rows)).astype(jnp.bfloat16)
        return carry

    lax.fori_loop(0, seqs // GROUP, close_group, 0)

    all_peaks().wait_send()
    msa_copy(0, 0, ms_sx, x_near, yline + 1).wait_send()
    for e in range(yline):
        pl.when(up_y & (y - e >= 0))(
            lambda: msa_copy(0, 0, ms_up.at[e], me_i + 2, 3).wait_send()
        )
        pl.when(down_y & (y + e < yline))(
            lambda: msa_copy(0, 0, ms_dn.at[e], me_i - 2, 3).wait_send()
        )
    pl.when(down_z)(lambda: ex_own_down().wait_send())

    def drain(c, carry):
        o = c * CORES + core
        ex_mate(o).wait_send()
        pl.when((c <= z) & up_z)(lambda: ex_up(o).wait_send())
        pl.when((c > z) & down_z)(lambda: ex_down(o).wait_send())
        return carry

    lax.fori_loop(0, line, drain, 0)


def body(pi_count, pj_count, duo, duo_w, aligned, gain, shift, payload_w, switch_w, closing_w):
    rows, cols, pair_chans = duo.shape
    seqs, chans, tokens = aligned.shape
    heads, joint = duo_w.shape[1], payload_w.shape[1]
    span = seqs * (joint // heads)
    chunks = rows // CHUNK
    assert tokens == rows == CORES * cols and pj_count == CORES * pi_count
    assert pi_count >= 4 and pi_count >= chunks // 2
    vmem = pl.BlockSpec(memory_space=pltpu.VMEM)
    hbm = pl.BlockSpec(memory_space=pltpu.HBM)
    dma = pltpu.SemaphoreType.DMA
    return pl.pallas_call(
        functools.partial(kernel, pi_count, pj_count),
        in_specs=[hbm, vmem, hbm] + [vmem] * 5,
        out_specs=vmem,
        out_shape=pltpu.VMEM(aligned.shape, jnp.bfloat16),
        scratch_shapes=[
            pltpu.VMEM((joint, chans), jnp.bfloat16),
            pltpu.VMEM((joint, chans), jnp.bfloat16),
            pltpu.VMEM((2, chans, rows), jnp.float32),
            pltpu.VMEM((chunks, CHUNK, cols, pair_chans), jnp.bfloat16),
            pltpu.VMEM((pi_count * 2, seqs // 2, chans, tokens), jnp.bfloat16),
            pltpu.VMEM((pj_count, chunks, heads, CHUNK, cols), jnp.bfloat16),
            pltpu.VMEM((heads, CHUNK, cols), jnp.float32),
            pltpu.VMEM((pj_count, heads, rows), jnp.float32),
            pltpu.VMEM((pj_count, heads, rows), jnp.float32),
            pltpu.VMEM((2, heads, span + 16, rows), jnp.bfloat16),
            pltpu.VMEM((3, heads, rows, CORES * cols), jnp.bfloat16),
            pltpu.VMEM((heads, span + 16, rows), jnp.float32),
            pltpu.VMEM((seqs, joint, tokens), jnp.float32),
            dma((chunks,)),
            dma((2,)),
            dma((pj_count // CORES, chunks)),
            dma((pj_count // CORES,)),
            dma,
            dma((pj_count // CORES,)),
            dma((pj_count // CORES,)),
            dma,
            dma,
            dma((pi_count, 2)),
            dma,
            dma((pi_count // 2,)),
            dma((pi_count // 2,)),
        ],
        compiler_params=pltpu.CompilerParams(
            collective_id=0, has_side_effects=True, vmem_limit_bytes=VMEM_LIMIT
        ),
        name="layer",
    )(
        duo,
        duo_w.T,
        aligned,
        gain[None, :],
        shift[None, :],
        payload_w,
        switch_w,
        closing_w.T,
    )


def solution(mesh):
    return jax.shard_map(
        functools.partial(body, mesh.shape["pi"], mesh.shape["pj"]),
        mesh=mesh,
        in_specs=(P("pi", "pj", None), P(), P("pj", None, "pi"), P(), P(), P(), P(), P()),
        out_specs=P("pj", None, "pi"),
        check_vma=False,
    )
```

```python
import functools

import jax
import jax.numpy as jnp
from jax import lax
from jax.experimental import pallas as pl
from jax.experimental.pallas import tpu as pltpu
from jax.sharding import PartitionSpec as P

EPS = 1e-05
MESH = pl.DeviceIdType.MESH
NT = (((1,), (1,)), ((), ()))
CORES = 2
TILE = 16
CHUNK = 32
GROUP = 16
AHEAD = 3
SLOTS = 4
HELD = 3
VMEM_LIMIT = 61 << 20


def dot(a, b, dims=(((1,), (0,)), ((), ()))):
    return lax.dot_general(a, b, dims, preferred_element_type=jnp.float32)


def split_weights(w):
    w = w - jnp.mean(w, axis=1, keepdims=True)
    hi = w.astype(jnp.bfloat16).astype(jnp.float32)
    mid = (w - hi).astype(jnp.bfloat16).astype(jnp.float32)
    w3 = jnp.concatenate([hi, mid, w - hi - mid, jnp.zeros_like(w)], axis=0)
    return w3.astype(jnp.bfloat16)


def tile_scores(x, w3, centring):
    rows, cols, chans = x.shape
    heads = w3.shape[0] // 4
    x = x.reshape(rows * cols, chans)
    half = rows * cols // 2
    centred = dot(jnp.concatenate([x[:half], x[half:]], axis=1), centring)
    square = centred * centred
    one, two = square[:, :chans], square[:, chans:]
    lane = lax.broadcasted_iota(jnp.int32, one.shape, 1)
    low = lane < chans // 2
    both = jnp.where(low, one, two) + pltpu.roll(jnp.where(low, two, one), chans // 2, 1)
    one, two = both[: half // 2], both[half // 2 :]
    quarter = chans // 4
    low = lane[: half // 2] % (2 * quarter) < quarter
    both = jnp.where(
        low, one + pltpu.roll(one, chans - quarter, 1), two + pltpu.roll(two, quarter, 1)
    )
    top = both.astype(jnp.bfloat16)
    rest = (both - top.astype(jnp.float32)).astype(jnp.bfloat16)
    group = lax.broadcasted_iota(jnp.int32, (4 * heads, 2 * chans), 0) // heads
    owner = lax.broadcasted_iota(jnp.int32, (4 * heads, 2 * chans), 1) % chans // quarter
    picks = jnp.where(group == owner, 1.0, 0.0).astype(jnp.bfloat16)
    sums = dot(picks, jnp.concatenate([top, rest], axis=1), NT)
    sums = [sums[g * heads : (g + 1) * heads] for g in range(4)]
    variance = jnp.concatenate(sums, axis=1) * (1.0 / chans)
    parts = dot(w3, x, NT)
    scores = parts[:heads] + (parts[heads : 2 * heads] + parts[2 * heads : 3 * heads])
    return scores * lax.rsqrt(variance + EPS)


def kernel(
    pi_count,
    pj_count,
    pair_hbm,
    w_ref,
    msa_hbm,
    gain_ref,
    shift_ref,
    payload_ref,
    switch_ref,
    wc_ref,
    out_ref,
    wv_ref,
    ws_ref,
    spread,
    centring,
    pair,
    msa,
    ex,
    hold,
    peaks,
    turned,
    vals,
    weights,
    acc,
    gate,
    pair_sem,
    msa_sem,
    ex_rs,
    ex_fw,
    ex_dn,
    ex_pt,
    ex_far,
    pk_rs,
    pk_ss,
    ms_rs,
    ms_sx,
    ms_up,
    ms_dn,
    rounds,
):
    me_i, me_j = lax.axis_index("pi"), lax.axis_index("pj")
    line, yline = pj_count // CORES, pi_count // 2
    z, core = me_j // CORES, me_j % CORES
    y, x = me_i // 2, me_i % 2
    chunks = ex.shape[1]
    heads, cols = ex.shape[2], ex.shape[4]
    rows = chunks * CHUNK
    seqs, half, chans = out_ref.shape[0], msa.shape[1], msa.shape[2]
    span = vals.shape[2] - 16
    width = span // seqs
    mate = me_j - core + (1 - core)
    x_near = me_i - x + (1 - x)

    pair_in = lambda q: pltpu.make_async_copy(
        pair_hbm.at[pl.ds(q * CHUNK, CHUNK)], pair.at[q % AHEAD], pair_sem.at[q % AHEAD]
    )
    own_in = [
        pltpu.make_async_copy(msa_hbm.at[pl.ds(h * half, half)], msa.at[me_i * 2 + h], msa_sem.at[h])
        for h in range(2)
    ]
    for h in range(2):
        own_in[h].start()
    lax.fori_loop(0, AHEAD, lambda q, c: (pair_in(q).start(), c)[1], 0)

    barrier = pltpu.get_barrier_semaphore()

    def greet(i, j):
        pl.semaphore_signal(barrier, inc=1, device_id=(i, j), device_id_type=MESH)

    up_y, down_y = y < yline - 1, y > 0
    up_z, down_z = z < line - 1, z > 0
    near_z = 1 + jnp.where(up_z, 1, 0) + jnp.where(down_z, 1, 0)
    near_y = jnp.where(up_y, 1, 0) + jnp.where(down_y, 1, 0)

    def tell_line(tell):
        tell(me_i, mate)
        pl.when(up_z)(lambda: tell(me_i, me_j + CORES))
        pl.when(down_z)(lambda: tell(me_i, me_j - CORES))

    tell_line(greet)
    greet(x_near, me_j)
    pl.when(up_y)(lambda: greet(me_i + 2, me_j))
    pl.when(down_y)(lambda: greet(me_i - 2, me_j))

    pl.semaphore_wait(barrier, 1 + near_y + near_z)

    def msa_copy(p, h, send, i, count=1):
        part = msa.at[pl.ds(p * 2 + h, count)]
        return pltpu.make_async_remote_copy(
            part, part, send, ms_rs.at[p, h], device_id=(i, me_j), device_id_type=MESH
        )

    def to_x(p, h):
        return msa_copy(p, h, ms_sx, x_near)

    def to_up(p, h, e):
        return msa_copy(p, h, ms_up.at[e], me_i + 2)

    def to_down(p, h, e):
        return msa_copy(p, h, ms_dn.at[e], me_i - 2)

    def along_y(p, h):
        pl.when(up_y)(lambda: to_up(p, h, 0).start())
        pl.when(down_y)(lambda: to_down(p, h, 0).start())

    def take(p, h):
        to_x(p, h).wait_recv()

    for h in range(2):
        own_in[h].wait()
    to_x(me_i, 0).start()
    along_y(me_i, 1)
    to_x(me_i, 1).start()
    along_y(me_i, 0)

    def pass_y(e, column, h, cross):
        below, above = me_i - x + column - 2 * e, me_i - x + column + 2 * e

        @pl.when(y - e >= 0)
        def _():
            take(below, h)
            pl.when(up_y)(lambda: to_up(below, h, e).start())
            if cross:
                to_x(below, h).start()

        @pl.when(y + e < yline)
        def _():
            take(above, h)
            pl.when(down_y)(lambda: to_down(above, h, e).start())
            if cross:
                to_x(above, h).start()

    def first_relays():
        take(x_near, 0)
        along_y(x_near, 0)
        for e in range(1, yline):
            pass_y(e, x, 1, True)

    def ex_copy(o, q, send, receive, j):
        block = ex.at[o] if q is None else ex.at[o, q]
        return pltpu.make_async_remote_copy(
            block, block, send, receive, device_id=(me_i, j), device_id_type=MESH
        )

    def ex_along(o, q, send, j):
        c = o // CORES
        return ex_copy(o, q, send, ex_rs.at[c, 0 if q is None else q], j)

    def ex_up(o, q=None):
        return ex_along(o, q, ex_fw.at[o // CORES], me_j + CORES)

    def ex_down(o, q=None):
        return ex_along(o, q, ex_fw.at[o // CORES], me_j - CORES)

    def ex_own_down(q=None):
        return ex_along(me_j, q, ex_dn, me_j - CORES)

    def ex_mate(o, q=None):
        late = 0 if q is None else jnp.where(q >= chunks - HELD, 1, 0)
        return ex_copy(o, q, ex_pt.at[o // CORES], ex_far.at[o // CORES, late], mate)

    def ex_mate_part(o, late):
        block = ex.at[o, pl.ds(chunks - HELD, HELD) if late else pl.ds(0, chunks - HELD)]
        c = o // CORES
        return pltpu.make_async_remote_copy(
            block, block, ex_pt.at[c], ex_far.at[c, late], device_id=(me_i, mate), device_id_type=MESH
        )

    def send_own(q):
        pl.when(up_z)(lambda: ex_up(me_j, q).start())
        pl.when(down_z)(lambda: ex_own_down(q).start())
        ex_mate(me_j, q).start()

    def relay(d, q):
        below, above = me_j - CORES * d, me_j + CORES * d

        @pl.when(z - d >= 0)
        def _():
            ex_up(below, q).wait_recv()
            pl.when(up_z)(lambda: ex_up(below, q).start())
            ex_mate(below, q).start()

        @pl.when(z + d < line)
        def _():
            ex_up(above, q).wait_recv()
            pl.when(down_z)(lambda: ex_down(above, q).start())
            ex_mate(above, q).start()

    def peak_copy(o, j):
        return pltpu.make_async_remote_copy(
            peaks.at[o], peaks.at[o], pk_ss, pk_rs,
            device_id=(me_i, j), device_id_type=MESH,
        )

    def all_peaks():
        part = peaks.at[pl.ds(0, pj_count - 1)]
        return pltpu.make_async_remote_copy(
            part, part, pk_ss, pk_rs, device_id=(me_i, mate), device_id_type=MESH
        )

    def others(f):
        lax.fori_loop(1, pj_count, lambda r, c: (f((me_j + r) % pj_count), c)[1], 0)

    def tell_round(r):
        def tell(i, j):
            pl.semaphore_signal(rounds.at[r], inc=1, device_id=(i, j), device_id_type=MESH)

        tell_line(tell)

    def hear_round(r):
        pl.semaphore_wait(rounds.at[r], near_z)

    tell_round(0)
    w3 = split_weights(w_ref[...])
    pair_chans = w3.shape[1]
    across = lax.broadcasted_iota(jnp.int32, centring.shape, 0)
    along = lax.broadcasted_iota(jnp.int32, centring.shape, 1)
    away = jnp.where(across // pair_chans == along // pair_chans, -1.0 / pair_chans, 0.0)
    centring[...] = jnp.where(across == along, 1.0 + away, away).astype(jnp.bfloat16)
    lane = lax.broadcasted_iota(jnp.int32, (heads, rows), 1)
    peaks[me_j] = jnp.zeros((heads, rows), jnp.float32)

    def pair_chunk(q):
        pair_in(q).wait()
        top = peaks[me_j]
        for t in range(CHUNK // TILE):
            scores = tile_scores(pair[q % AHEAD, t * TILE : (t + 1) * TILE], w3, centring[...])
            for k in range(TILE):
                one = scores[:, k * cols : (k + 1) * cols]
                peak = jnp.max(one, axis=1, keepdims=True)
                hold[:, t * TILE + k, :] = jnp.exp(one - peak)
                top = jnp.where(lane == q * CHUNK + t * TILE + k, peak, top)
        peaks[me_j] = top
        ex[me_j, q] = hold[...].astype(jnp.bfloat16)
        pl.when(q + AHEAD < chunks)(lambda: pair_in(q + AHEAD).start())

    def pair_step(q, carry):
        pair_chunk(q)
        send_own(q)

        @pl.when(q < line - 1)
        def _():
            hear_round(q)
            pl.when(q < line - 2)(lambda: tell_round(q + 1))

        return carry

    lax.fori_loop(0, chunks, pair_step, 0)
    others(lambda j: peak_copy(me_j, j).start())

    def relays(d, first, last):
        lax.fori_loop(first, last, lambda q, c: (relay(d, q), c)[1], 0)

    def normed(p, s):
        v = msa[p * 2 + s // half, s % half].astype(jnp.float32)
        v = v - jnp.mean(v, axis=0, keepdims=True)
        variance = jnp.mean(v * v, axis=0, keepdims=True)
        return (v * lax.rsqrt(variance + EPS) * spread[0] + spread[1]).astype(jnp.bfloat16)

    def gate_group(g, carry):
        for k in range(GROUP):
            s = g * GROUP + k
            gate[s] = jax.nn.sigmoid(dot(ws_ref[...], normed(me_i, s)))
        return carry

    wv_ref[...] = payload_ref[...].astype(jnp.float32).T.astype(jnp.bfloat16)
    ws_ref[...] = switch_ref[...].astype(jnp.float32).T.astype(jnp.bfloat16)
    diagonal = lax.broadcasted_iota(jnp.int32, (chans, chans), 0)
    diagonal = diagonal == lax.broadcasted_iota(jnp.int32, (chans, chans), 1)
    for k, ref in enumerate((gain_ref, shift_ref)):
        column = jnp.sum(jnp.where(diagonal, ref[...], 0.0), axis=1, keepdims=True)
        spread[k] = jnp.broadcast_to(column, (chans, rows))

    relays(1, 0, chunks - 2)
    lax.fori_loop(0, seqs // GROUP, gate_group, 0)
    relays(1, chunks - 2, chunks)
    first_relays()

    for slot in range(SLOTS):
        vals[slot, :, span:, :] = jnp.ones((heads, 16, rows), jnp.bfloat16)

    def zero_head(h, carry):
        acc[h] = jnp.zeros(acc.shape[1:], jnp.float32)
        return carry

    lax.fori_loop(0, heads, zero_head, 0)

    def values(p, h, slot):
        def value_group(g, carry):
            for k in range(GROUP):
                s = g * GROUP + k
                v = dot(wv_ref[...], normed(p, s)).astype(jnp.bfloat16)
                at = pl.ds(pl.multiple_of(s * width, width), width)
                for n in range(heads):
                    vals[slot, n, at, :] = v[n * width : (n + 1) * width]
            return carry

        steps = half // GROUP
        lax.fori_loop(h * steps, (h + 1) * steps, value_group, 0)

    y_near = (y + 1) % yline * 2 + x

    def slot_of(p):
        return jnp.where(p == me_i, 0, jnp.where(p == x_near, 1, jnp.where(p == y_near, 2, 3)))

    def early_values(k, carry):
        p = jnp.where(k < 2, me_i, jnp.where(k == 2, x_near, y_near))
        h = jnp.where((k == 1) | (k == 3), 1, 0)
        values(p, h, slot_of(p))
        return carry

    lax.fori_loop(0, 4, early_values, 0)

    all_peaks().wait_recv()
    top = jnp.max(peaks[...], axis=0)

    def turn(o, carry):
        pad = jnp.zeros((128 - heads, rows), jnp.float32)
        turned[o] = jnp.concatenate([jnp.exp(peaks[o] - top), pad], axis=0).T
        return carry

    lax.fori_loop(0, pj_count, turn, 0)

    def rescale(p, slot, late):
        first, last = (chunks - HELD, chunks) if late else (0, chunks - HELD)
        ex_mate_part(p * CORES + (1 - core), late).wait_recv()
        span_rows = slice(first * CHUNK, last * CHUNK)
        for c in range(CORES):
            o = p * CORES + c
            for h in range(heads):
                e = ex[o, first:last, h].reshape((last - first) * CHUNK, cols).astype(jnp.float32)
                e = (e * turned[o, span_rows, h : h + 1]).astype(jnp.bfloat16)
                weights[slot, h, span_rows, c * cols : (c + 1) * cols] = e

    def attend(slot, weight_slot):
        for h in range(heads):
            acc[h] += dot(vals[slot, h], weights[weight_slot, h], NT)

    def apart(p):
        return jnp.where(p > z, p - z, z - p)

    def crosses(p):
        return (p // 2 != y) & (p % 2 != x)

    def attend_unit(p):
        near = jnp.where(apart(p) <= 1, jnp.where(p == me_i, 0, 1), apart(p))
        unit = jnp.where(crosses(p), line - 1, near)
        return jnp.where(apart(p) == line - 1, line, unit)

    def value_unit(p):
        late = line - 1 if pi_count <= SLOTS else attend_unit(p)
        late = jnp.where(crosses(p), late, attend_unit(p))
        return jnp.where(p == me_i, -1, jnp.where((p == x_near) | (p == y_near), 1, late))

    half_way = chunks // 2
    diagonal_block = (y + 1) % yline * 2 + (1 - x)

    def step(n, carry):
        u, p = n // pi_count, n % pi_count
        fresh = p == 0

        @pl.when(fresh & (u == 1))
        def _():
            relays(2, 0, half_way)
            for e in range(1, yline):
                pass_y(e, x, 0, False)

        @pl.when((u == 1) & (p < chunks - half_way))
        def _():
            relay(2, half_way + p)

        @pl.when(fresh & (u >= 3) & (u < line - 1))
        def _():
            relays(u, 0, chunks)

        @pl.when(fresh & (u == line - 1))
        def _():
            relays(line - 1, 0, chunks - HELD)
            farthest = jnp.where(z == 0, line - 1, 0)
            pl.when((z == 0) | (z == line - 1))(lambda: rescale(farthest, 1, 0))
            for e in range(1, yline):
                pass_y(e, 1 - x, 0, False)

        last = apart(p) == line - 1
        early = (p == diagonal_block) & jnp.logical_not(last)
        weight_slot = jnp.where(early, 2, jnp.where(last, 1, 0))
        rescale_unit = jnp.where(early, line - 2, attend_unit(p))

        @pl.when(value_unit(p) == u)
        def _():
            pl.when(p % 2 != x)(lambda: take(p, 1))
            first = jnp.where(p == x_near, 1, 0)
            end = jnp.where(p == y_near, 1, 2)
            lax.fori_loop(first, end, lambda h, c: (values(p, h, slot_of(p)), c)[1], 0)

        @pl.when((u == line - 1) & (p == diagonal_block))
        def _():
            relays(line - 1, chunks - HELD, chunks)

        @pl.when(rescale_unit == u)
        def _():
            pl.when(jnp.logical_not(last))(lambda: rescale(p, weight_slot, 0))
            rescale(p, weight_slot, 1)

        pl.when(attend_unit(p) == u)(lambda: attend(slot_of(p), weight_slot))
        return carry

    lax.fori_loop(0, (line + 1) * pi_count, step, 0)

    inverse = 1.0 / acc[:, span : span + 8, :]
    inverse = inverse[:, :1, :]

    def close_group(g, carry):
        for k in range(GROUP):
            s = g * GROUP + k
            at = pl.ds(pl.multiple_of(s * width, width), width)
            share = gate[s].reshape(heads, width, rows)
            mixed = (share * (acc[:, at, :] * inverse)).astype(jnp.bfloat16)
            out_ref[s] = dot(wc_ref[...], mixed.reshape(heads * width, rows)).astype(jnp.bfloat16)
        return carry

    lax.fori_loop(0, seqs // GROUP, close_group, 0)

    all_peaks().wait_send()
    msa_copy(0, 0, ms_sx, x_near, yline + 1).wait_send()
    for e in range(yline):
        pl.when(up_y & (y - e >= 0))(
            lambda: msa_copy(0, 0, ms_up.at[e], me_i + 2, 3).wait_send()
        )
        pl.when(down_y & (y + e < yline))(
            lambda: msa_copy(0, 0, ms_dn.at[e], me_i - 2, 3).wait_send()
        )
    pl.when(down_z)(lambda: ex_own_down().wait_send())

    def drain(c, carry):
        o = c * CORES + core
        ex_mate(o).wait_send()
        pl.when((c <= z) & up_z)(lambda: ex_up(o).wait_send())
        pl.when((c > z) & down_z)(lambda: ex_down(o).wait_send())
        return carry

    lax.fori_loop(0, line, drain, 0)


def body(pi_count, pj_count, duo, duo_w, aligned, gain, shift, payload_w, switch_w, closing_w):
    rows, cols, pair_chans = duo.shape
    seqs, chans, tokens = aligned.shape
    heads, joint = duo_w.shape[1], payload_w.shape[1]
    span = seqs * (joint // heads)
    chunks = rows // CHUNK
    assert tokens == rows == CORES * cols and pj_count == CORES * pi_count
    assert pi_count >= 4 and pi_count >= chunks // 2
    vmem = pl.BlockSpec(memory_space=pltpu.VMEM)
    hbm = pl.BlockSpec(memory_space=pltpu.HBM)
    dma = pltpu.SemaphoreType.DMA
    return pl.pallas_call(
        functools.partial(kernel, pi_count, pj_count),
        in_specs=[hbm, vmem, hbm] + [vmem] * 5,
        out_specs=vmem,
        out_shape=pltpu.VMEM(aligned.shape, jnp.bfloat16),
        scratch_shapes=[
            pltpu.VMEM((joint, chans), jnp.bfloat16),
            pltpu.VMEM((joint, chans), jnp.bfloat16),
            pltpu.VMEM((2, chans, rows), jnp.float32),
            pltpu.VMEM((2 * pair_chans, 2 * pair_chans), jnp.bfloat16),
            pltpu.VMEM((AHEAD, CHUNK, cols, pair_chans), jnp.bfloat16),
            pltpu.VMEM((pi_count * 2, seqs // 2, chans, tokens), jnp.bfloat16),
            pltpu.VMEM((pj_count, chunks, heads, CHUNK, cols), jnp.bfloat16),
            pltpu.VMEM((heads, CHUNK, cols), jnp.float32),
            pltpu.VMEM((pj_count, heads, rows), jnp.float32),
            pltpu.VMEM((pj_count, rows, 128), jnp.float32),
            pltpu.VMEM((SLOTS, heads, span + 16, rows), jnp.bfloat16),
            pltpu.VMEM((3, heads, rows, CORES * cols), jnp.bfloat16),
            pltpu.VMEM((heads, span + 16, rows), jnp.float32),
            pltpu.VMEM((seqs, joint, tokens), jnp.float32),
            dma((AHEAD,)),
            dma((2,)),
            dma((pj_count // CORES, chunks)),
            dma((pj_count // CORES,)),
            dma,
            dma((pj_count // CORES,)),
            dma((pj_count // CORES, 2)),
            dma,
            dma,
            dma((pi_count, 2)),
            dma,
            dma((pi_count // 2,)),
            dma((pi_count // 2,)),
            pltpu.SemaphoreType.REGULAR((pj_count // CORES - 1,)),
        ],
        compiler_params=pltpu.CompilerParams(
            collective_id=0, has_side_effects=True, vmem_limit_bytes=VMEM_LIMIT
        ),
        name="layer",
    )(
        duo,
        duo_w.T,
        aligned,
        gain[None, :],
        shift[None, :],
        payload_w,
        switch_w,
        closing_w.T,
    )


def solution(mesh):
    return jax.shard_map(
        functools.partial(body, mesh.shape["pi"], mesh.shape["pj"]),
        mesh=mesh,
        in_specs=(P("pi", "pj", None), P(), P("pj", None, "pi"), P(), P(), P(), P(), P()),
        out_specs=P("pj", None, "pi"),
        check_vma=False,
    )
```

```python
import functools

import jax
import jax.numpy as jnp
from jax import lax
from jax.experimental import pallas as pl
from jax.experimental.pallas import tpu as pltpu
from jax.sharding import PartitionSpec as P

EPS = 1e-05
MESH = pl.DeviceIdType.MESH
NT = (((1,), (1,)), ((), ()))
CORES = 2
TILE = 16
PIECE = 32
CHUNK = 32
GROUP = 16
AHEAD = 3
SLOTS = 4
SOON = 5
HELD = 3
VMEM_LIMIT = 61 << 20


def dot(a, b, dims=(((1,), (0,)), ((), ()))):
    return lax.dot_general(a, b, dims, preferred_element_type=jnp.float32)


def split_weights(w):
    w = w - jnp.mean(w, axis=1, keepdims=True)
    hi = w.astype(jnp.bfloat16).astype(jnp.float32)
    mid = (w - hi).astype(jnp.bfloat16).astype(jnp.float32)
    w3 = jnp.concatenate([hi, mid, w - hi - mid, jnp.zeros_like(w)], axis=0)
    return w3.astype(jnp.bfloat16)


def tile_scores(x, w3, centring):
    rows, cols, chans = x.shape
    heads = w3.shape[0] // 4
    x = x.reshape(rows * cols, chans)
    half = rows * cols // 2
    centred = dot(jnp.concatenate([x[:half], x[half:]], axis=1), centring)
    square = centred * centred
    one, two = square[:, :chans], square[:, chans:]
    lane = lax.broadcasted_iota(jnp.int32, one.shape, 1)
    low = lane < chans // 2
    both = jnp.where(low, one, two) + pltpu.roll(jnp.where(low, two, one), chans // 2, 1)
    one, two = both[: half // 2], both[half // 2 :]
    quarter = chans // 4
    low = lane[: half // 2] % (2 * quarter) < quarter
    both = jnp.where(
        low, one + pltpu.roll(one, chans - quarter, 1), two + pltpu.roll(two, quarter, 1)
    )
    top = both.astype(jnp.bfloat16)
    rest = (both - top.astype(jnp.float32)).astype(jnp.bfloat16)
    group = lax.broadcasted_iota(jnp.int32, (4 * heads, 2 * chans), 0) // heads
    owner = lax.broadcasted_iota(jnp.int32, (4 * heads, 2 * chans), 1) % chans // quarter
    picks = jnp.where(group == owner, 1.0, 0.0).astype(jnp.bfloat16)
    sums = dot(picks, jnp.concatenate([top, rest], axis=1), NT)
    sums = [sums[g * heads : (g + 1) * heads] for g in range(4)]
    variance = jnp.concatenate(sums, axis=1) * (1.0 / chans)
    parts = dot(w3, x, NT)
    scores = parts[:heads] + (parts[heads : 2 * heads] + parts[2 * heads : 3 * heads])
    return scores * lax.rsqrt(variance + EPS)


def kernel(
    pi_count,
    pj_count,
    pair_hbm,
    w_hbm,
    msa_hbm,
    gain_hbm,
    shift_hbm,
    payload_hbm,
    switch_hbm,
    wc_hbm,
    out_ref,
    w_ref,
    gain_ref,
    shift_ref,
    payload_ref,
    switch_ref,
    wc_ref,
    wv_ref,
    ws_ref,
    spread,
    centring,
    pair,
    msa,
    ex,
    hold,
    peaks,
    turned,
    vals,
    weights,
    acc,
    gate,
    w_sem,
    small_sem,
    pair_sem,
    msa_sem,
    ex_rs,
    ex_fw,
    ex_dn,
    ex_pt,
    ex_far,
    pk_rs,
    pk_ss,
    ms_rs,
    ms_sx,
    ms_up,
    ms_dn,
    rounds,
):
    me_i, me_j = lax.axis_index("pi"), lax.axis_index("pj")
    line, yline = pj_count // CORES, pi_count // 2
    z, core = me_j // CORES, me_j % CORES
    y, x = me_i // 2, me_i % 2
    chunks = ex.shape[1]
    heads, cols = ex.shape[2], ex.shape[4]
    rows = chunks * CHUNK
    share = CHUNK // PIECE
    seqs, half, chans = out_ref.shape[0], msa.shape[1], msa.shape[2]
    span = vals.shape[2] - 16
    width = span // seqs
    mate = me_j - core + (1 - core)
    x_near = me_i - x + (1 - x)

    pair_in = lambda q: pltpu.make_async_copy(
        pair_hbm.at[pl.ds(q * PIECE, PIECE)], pair.at[q % AHEAD], pair_sem.at[q % AHEAD]
    )
    own_in = [
        pltpu.make_async_copy(msa_hbm.at[pl.ds(h * half, half)], msa.at[me_i * 2 + h], msa_sem.at[h])
        for h in range(2)
    ]
    w_in = pltpu.make_async_copy(w_hbm, w_ref, w_sem)
    w_in.start()
    for h in range(2):
        own_in[h].start()
    lax.fori_loop(0, AHEAD, lambda q, c: (pair_in(q).start(), c)[1], 0)
    small_in = [
        pltpu.make_async_copy(source, target, small_sem.at[k])
        for k, (source, target) in enumerate(
            (
                (gain_hbm, gain_ref),
                (shift_hbm, shift_ref),
                (payload_hbm, payload_ref),
                (switch_hbm, switch_ref),
                (wc_hbm, wc_ref),
            )
        )
    ]
    for copy in small_in:
        copy.start()

    barrier = pltpu.get_barrier_semaphore()

    def greet(i, j):
        pl.semaphore_signal(barrier, inc=1, device_id=(i, j), device_id_type=MESH)

    up_y, down_y = y < yline - 1, y > 0
    up_z, down_z = z < line - 1, z > 0
    near_z = 1 + jnp.where(up_z, 1, 0) + jnp.where(down_z, 1, 0)
    near_y = jnp.where(up_y, 1, 0) + jnp.where(down_y, 1, 0)

    def tell_line(tell):
        tell(me_i, mate)
        pl.when(up_z)(lambda: tell(me_i, me_j + CORES))
        pl.when(down_z)(lambda: tell(me_i, me_j - CORES))

    tell_line(greet)
    greet(x_near, me_j)
    pl.when(up_y)(lambda: greet(me_i + 2, me_j))
    pl.when(down_y)(lambda: greet(me_i - 2, me_j))

    pl.semaphore_wait(barrier, 1 + near_y + near_z)

    def msa_copy(p, h, send, i, count=1):
        part = msa.at[pl.ds(p * 2 + h, count)]
        return pltpu.make_async_remote_copy(
            part, part, send, ms_rs.at[p, h], device_id=(i, me_j), device_id_type=MESH
        )

    def to_x(p, h):
        return msa_copy(p, h, ms_sx, x_near)

    def to_up(p, h, e):
        return msa_copy(p, h, ms_up.at[e], me_i + 2)

    def to_down(p, h, e):
        return msa_copy(p, h, ms_dn.at[e], me_i - 2)

    def along_y(p, h):
        pl.when(up_y)(lambda: to_up(p, h, 0).start())
        pl.when(down_y)(lambda: to_down(p, h, 0).start())

    def take(p, h):
        to_x(p, h).wait_recv()

    for h in range(2):
        own_in[h].wait()
    to_x(me_i, 0).start()
    along_y(me_i, 1)
    to_x(me_i, 1).start()
    along_y(me_i, 0)

    def pass_y(e, column, h, cross):
        below, above = me_i - x + column - 2 * e, me_i - x + column + 2 * e

        @pl.when(y - e >= 0)
        def _():
            take(below, h)
            pl.when(up_y)(lambda: to_up(below, h, e).start())
            if cross:
                to_x(below, h).start()

        @pl.when(y + e < yline)
        def _():
            take(above, h)
            pl.when(down_y)(lambda: to_down(above, h, e).start())
            if cross:
                to_x(above, h).start()

    def first_relays():
        take(x_near, 0)
        along_y(x_near, 0)
        for e in range(1, yline):
            pass_y(e, x, 1, True)

    def ex_copy(o, q, send, receive, j):
        block = ex.at[o] if q is None else ex.at[o, q]
        return pltpu.make_async_remote_copy(
            block, block, send, receive, device_id=(me_i, j), device_id_type=MESH
        )

    def ex_along(o, q, send, j):
        c = o // CORES
        return ex_copy(o, q, send, ex_rs.at[c, 0 if q is None else q], j)

    def ex_up(o, q=None):
        return ex_along(o, q, ex_fw.at[o // CORES], me_j + CORES)

    def ex_down(o, q=None):
        return ex_along(o, q, ex_fw.at[o // CORES], me_j - CORES)

    def ex_own_down(q=None):
        return ex_along(me_j, q, ex_dn, me_j - CORES)

    def ex_mate(o, q=None):
        late = 0 if q is None else jnp.where(q >= chunks - HELD, 1, 0)
        return ex_copy(o, q, ex_pt.at[o // CORES], ex_far.at[o // CORES, late], mate)

    def ex_mate_part(o, late):
        block = ex.at[o, pl.ds(chunks - HELD, HELD) if late else pl.ds(0, chunks - HELD)]
        c = o // CORES
        return pltpu.make_async_remote_copy(
            block, block, ex_pt.at[c], ex_far.at[c, late], device_id=(me_i, mate), device_id_type=MESH
        )

    def send_own(q):
        pl.when(up_z)(lambda: ex_up(me_j, q).start())
        pl.when(down_z)(lambda: ex_own_down(q).start())
        ex_mate(me_j, q).start()

    def relay(d, q):
        below, above = me_j - CORES * d, me_j + CORES * d

        @pl.when(z - d >= 0)
        def _():
            ex_up(below, q).wait_recv()
            pl.when(up_z)(lambda: ex_up(below, q).start())
            ex_mate(below, q).start()

        @pl.when(z + d < line)
        def _():
            ex_up(above, q).wait_recv()
            pl.when(down_z)(lambda: ex_down(above, q).start())
            ex_mate(above, q).start()

    def peak_copy(o, j):
        return pltpu.make_async_remote_copy(
            peaks.at[o], peaks.at[o], pk_ss, pk_rs,
            device_id=(me_i, j), device_id_type=MESH,
        )

    def all_peaks():
        part = peaks.at[pl.ds(0, pj_count - 1)]
        return pltpu.make_async_remote_copy(
            part, part, pk_ss, pk_rs, device_id=(me_i, mate), device_id_type=MESH
        )

    def others(f):
        lax.fori_loop(1, pj_count, lambda r, c: (f((me_j + r) % pj_count), c)[1], 0)

    def tell_round(r):
        def tell(i, j):
            pl.semaphore_signal(rounds.at[r], inc=1, device_id=(i, j), device_id_type=MESH)

        tell_line(tell)

    def hear_round(r):
        pl.semaphore_wait(rounds.at[r], near_z)

    tell_round(0)
    w_in.wait()
    w3 = split_weights(w_ref[...])
    pair_chans = w3.shape[1]
    across = lax.broadcasted_iota(jnp.int32, centring.shape, 0)
    along = lax.broadcasted_iota(jnp.int32, centring.shape, 1)
    away = jnp.where(across // pair_chans == along // pair_chans, -1.0 / pair_chans, 0.0)
    centring[...] = jnp.where(across == along, 1.0 + away, away).astype(jnp.bfloat16)
    lane = lax.broadcasted_iota(jnp.int32, (heads, rows), 1)
    peaks[me_j] = jnp.zeros((heads, rows), jnp.float32)

    def pair_piece(q):
        pair_in(q).wait()
        top = peaks[me_j]
        for t in range(PIECE // TILE):
            scores = tile_scores(pair[q % AHEAD, t * TILE : (t + 1) * TILE], w3, centring[...])
            for k in range(TILE):
                one = scores[:, k * cols : (k + 1) * cols]
                peak = jnp.max(one, axis=1, keepdims=True)
                hold[:, t * TILE + k, :] = jnp.exp(one - peak)
                top = jnp.where(lane == q * PIECE + t * TILE + k, peak, top)
        peaks[me_j] = top
        at = pl.ds(pl.multiple_of(q % share * PIECE, PIECE), PIECE)
        ex[me_j, q // share, :, at, :] = hold[...].astype(jnp.bfloat16)
        pl.when(q + AHEAD < chunks * share)(lambda: pair_in(q + AHEAD).start())

    soon = min(line - 1, (chunks * share - 2) // 2)

    def next_round(r):
        hear_round(r)
        pl.when(r < line - 2)(lambda: tell_round(r + 1))

    def pair_step(q, carry):
        pair_piece(q)
        pl.when(q % share == share - 1)(lambda: send_own(q // share))

        pl.when((q >= SOON) & (q % 2 == 1))(lambda: relay(1, (q - SOON) // 2))

        @pl.when((q % 2 == 1) & (q >= 3) & (q < 3 + 2 * soon))
        def _():
            next_round((q - 3) // 2)

        return carry

    lax.fori_loop(0, chunks * share, pair_step, 0)
    lax.fori_loop(soon, line - 1, lambda r, c: (next_round(r), c)[1], 0)
    others(lambda j: peak_copy(me_j, j).start())

    def relays(d, first, last):
        lax.fori_loop(first, last, lambda q, c: (relay(d, q), c)[1], 0)

    def normed(p, s):
        v = msa[p * 2 + s // half, s % half].astype(jnp.float32)
        v = v - jnp.mean(v, axis=0, keepdims=True)
        variance = jnp.mean(v * v, axis=0, keepdims=True)
        return (v * lax.rsqrt(variance + EPS) * spread[0] + spread[1]).astype(jnp.bfloat16)

    def gate_group(g, carry):
        for k in range(GROUP):
            s = g * GROUP + k
            gate[s] = jax.nn.sigmoid(dot(ws_ref[...], normed(me_i, s)))
        return carry

    for copy in small_in:
        copy.wait()
    wv_ref[...] = payload_ref[...].astype(jnp.float32).T.astype(jnp.bfloat16)
    ws_ref[...] = switch_ref[...].astype(jnp.float32).T.astype(jnp.bfloat16)
    diagonal = lax.broadcasted_iota(jnp.int32, (chans, chans), 0)
    diagonal = diagonal == lax.broadcasted_iota(jnp.int32, (chans, chans), 1)
    for k, ref in enumerate((gain_ref, shift_ref)):
        column = jnp.sum(jnp.where(diagonal, ref[...], 0.0), axis=1, keepdims=True)
        spread[k] = jnp.broadcast_to(column, (chans, rows))

    relays(1, (chunks - SOON + 1) // 2, chunks - 2)
    lax.fori_loop(0, seqs // GROUP, gate_group, 0)
    relays(1, chunks - 2, chunks)
    first_relays()

    for slot in range(SLOTS):
        vals[slot, :, span:, :] = jnp.ones((heads, 16, rows), jnp.bfloat16)

    def zero_head(h, carry):
        acc[h] = jnp.zeros(acc.shape[1:], jnp.float32)
        return carry

    lax.fori_loop(0, heads, zero_head, 0)

    def values(p, h, slot):
        def value_group(g, carry):
            for k in range(GROUP):
                s = g * GROUP + k
                v = dot(wv_ref[...], normed(p, s)).astype(jnp.bfloat16)
                at = pl.ds(pl.multiple_of(s * width, width), width)
                for n in range(heads):
                    vals[slot, n, at, :] = v[n * width : (n + 1) * width]
            return carry

        steps = half // GROUP
        lax.fori_loop(h * steps, (h + 1) * steps, value_group, 0)

    y_near = (y + 1) % yline * 2 + x

    def slot_of(p):
        return jnp.where(p == me_i, 0, jnp.where(p == x_near, 1, jnp.where(p == y_near, 2, 3)))

    def early_values(k, carry):
        p = jnp.where(k < 2, me_i, jnp.where(k == 2, x_near, y_near))
        h = jnp.where((k == 1) | (k == 3), 1, 0)
        values(p, h, slot_of(p))
        return carry

    lax.fori_loop(0, 4, early_values, 0)

    all_peaks().wait_recv()
    top = jnp.max(peaks[...], axis=0)

    def turn(o, carry):
        pad = jnp.zeros((128 - heads, rows), jnp.float32)
        turned[o] = jnp.concatenate([jnp.exp(peaks[o] - top), pad], axis=0).T
        return carry

    lax.fori_loop(0, pj_count, turn, 0)

    def rescale(p, slot, late):
        first, last = (chunks - HELD, chunks) if late else (0, chunks - HELD)
        ex_mate_part(p * CORES + (1 - core), late).wait_recv()
        span_rows = slice(first * CHUNK, last * CHUNK)
        for c in range(CORES):
            o = p * CORES + c
            for h in range(heads):
                e = ex[o, first:last, h].reshape((last - first) * CHUNK, cols).astype(jnp.float32)
                e = (e * turned[o, span_rows, h : h + 1]).astype(jnp.bfloat16)
                weights[slot, h, span_rows, c * cols : (c + 1) * cols] = e

    def attend(slot, weight_slot):
        for h in range(heads):
            acc[h] += dot(vals[slot, h], weights[weight_slot, h], NT)

    def apart(p):
        return jnp.where(p > z, p - z, z - p)

    def crosses(p):
        return (p // 2 != y) & (p % 2 != x)

    def farthest_from_here(p):
        return apart(p) == line - 1

    def attend_unit(p):
        near = jnp.where(apart(p) <= 1, jnp.where(p == me_i, 0, 1), apart(p))
        return jnp.where(crosses(p) | farthest_from_here(p), -1, near)

    def value_unit(p):
        beside = (p == x_near) | (p == y_near)
        return jnp.where(p == me_i, -1, jnp.where(beside, 1, attend_unit(p)))

    def late_values(p):
        pl.when(p % 2 != x)(lambda: take(p, 1))
        first = jnp.where(p == x_near, 1, 0)
        end = jnp.where(p == y_near, 1, 2)
        lax.fori_loop(first, end, lambda h, c: (values(p, h, slot_of(p)), c)[1], 0)

    half_way = chunks // 2
    diagonal_block = (y + 1) % yline * 2 + (1 - x)

    def step(n, carry):
        u, p = n // pi_count, n % pi_count
        fresh = p == 0

        @pl.when(fresh & (u == 1))
        def _():
            relays(2, 0, half_way)
            for e in range(1, yline):
                pass_y(e, x, 0, False)

        @pl.when((u == 1) & (p < chunks - half_way))
        def _():
            relay(2, half_way + p)

        @pl.when(fresh & (u >= 3))
        def _():
            relays(u, 0, chunks)

        pl.when(value_unit(p) == u)(lambda: late_values(p))

        @pl.when(attend_unit(p) == u)
        def _():
            rescale(p, 0, 0)
            rescale(p, 0, 1)
            attend(slot_of(p), 0)

        return carry

    lax.fori_loop(0, (line - 1) * pi_count, step, 0)

    at_end = (z == 0) | (z == line - 1)
    farthest = jnp.where(z == 0, line - 1, 0)

    @pl.when(jnp.logical_not(farthest_from_here(diagonal_block)))
    def _():
        rescale(diagonal_block, 2, 0)
        rescale(diagonal_block, 2, 1)

    relays(line - 1, 0, chunks - HELD)
    for e in range(1, yline):
        pass_y(e, 1 - x, 0, False)
    for e in range(1, yline):
        p = (y + e) % yline * 2 + (1 - x)
        here = jnp.logical_not(farthest_from_here(p))
        if pi_count <= SLOTS:
            late_values(p)
        else:
            pl.when(here)(lambda: late_values(p))
        if e == 1:
            relays(line - 1, chunks - HELD, chunks - 1)
            pl.when(at_end)(lambda: rescale(farthest, 1, 0))
            relay(line - 1, chunks - 1)

        @pl.when(here)
        def _():
            if e > 1:
                rescale(p, 0, 0)
                rescale(p, 0, 1)
            attend(slot_of(p), 2 if e == 1 else 0)

    @pl.when(at_end)
    def _():
        if pi_count > SLOTS:
            pl.when(slot_of(farthest) == 3)(lambda: late_values(farthest))
        rescale(farthest, 1, 1)
        attend(slot_of(farthest), 1)

    inverse = 1.0 / acc[:, span : span + 8, :]
    inverse = inverse[:, :1, :]

    def close_group(g, carry):
        for k in range(GROUP):
            s = g * GROUP + k
            at = pl.ds(pl.multiple_of(s * width, width), width)
            opened = gate[s].reshape(heads, width, rows)
            mixed = (opened * (acc[:, at, :] * inverse)).astype(jnp.bfloat16)
            out_ref[s] = dot(wc_ref[...], mixed.reshape(heads * width, rows)).astype(jnp.bfloat16)
        return carry

    lax.fori_loop(0, seqs // GROUP, close_group, 0)

    all_peaks().wait_send()
    msa_copy(0, 0, ms_sx, x_near, yline + 1).wait_send()
    for e in range(yline):
        pl.when(up_y & (y - e >= 0))(
            lambda: msa_copy(0, 0, ms_up.at[e], me_i + 2, 3).wait_send()
        )
        pl.when(down_y & (y + e < yline))(
            lambda: msa_copy(0, 0, ms_dn.at[e], me_i - 2, 3).wait_send()
        )
    pl.when(down_z)(lambda: ex_own_down().wait_send())

    def drain(c, carry):
        o = c * CORES + core
        ex_mate(o).wait_send()
        pl.when((c <= z) & up_z)(lambda: ex_up(o).wait_send())
        pl.when((c > z) & down_z)(lambda: ex_down(o).wait_send())
        return carry

    lax.fori_loop(0, line, drain, 0)


def body(pi_count, pj_count, duo, duo_w, aligned, gain, shift, payload_w, switch_w, closing_w):
    rows, cols, pair_chans = duo.shape
    seqs, chans, tokens = aligned.shape
    heads, joint = duo_w.shape[1], payload_w.shape[1]
    span = seqs * (joint // heads)
    chunks = rows // CHUNK
    assert tokens == rows == CORES * cols and pj_count == CORES * pi_count
    assert pi_count >= 4 and pi_count >= chunks // 2
    vmem = pl.BlockSpec(memory_space=pltpu.VMEM)
    hbm = pl.BlockSpec(memory_space=pltpu.HBM)
    dma = pltpu.SemaphoreType.DMA
    return pl.pallas_call(
        functools.partial(kernel, pi_count, pj_count),
        in_specs=[hbm] * 8,
        out_specs=vmem,
        out_shape=pltpu.VMEM(aligned.shape, jnp.bfloat16),
        scratch_shapes=[
            pltpu.VMEM((heads, pair_chans), jnp.float32),
            pltpu.VMEM((1, chans), jnp.float32),
            pltpu.VMEM((1, chans), jnp.float32),
            pltpu.VMEM(payload_w.shape, jnp.bfloat16),
            pltpu.VMEM(switch_w.shape, jnp.bfloat16),
            pltpu.VMEM(closing_w.shape[::-1], jnp.bfloat16),
            pltpu.VMEM((joint, chans), jnp.bfloat16),
            pltpu.VMEM((joint, chans), jnp.bfloat16),
            pltpu.VMEM((2, chans, rows), jnp.float32),
            pltpu.VMEM((2 * pair_chans, 2 * pair_chans), jnp.bfloat16),
            pltpu.VMEM((AHEAD, PIECE, cols, pair_chans), jnp.bfloat16),
            pltpu.VMEM((pi_count * 2, seqs // 2, chans, tokens), jnp.bfloat16),
            pltpu.VMEM((pj_count, chunks, heads, CHUNK, cols), jnp.bfloat16),
            pltpu.VMEM((heads, PIECE, cols), jnp.float32),
            pltpu.VMEM((pj_count, heads, rows), jnp.float32),
            pltpu.VMEM((pj_count, rows, 128), jnp.float32),
            pltpu.VMEM((SLOTS, heads, span + 16, rows), jnp.bfloat16),
            pltpu.VMEM((3, heads, rows, CORES * cols), jnp.bfloat16),
            pltpu.VMEM((heads, span + 16, rows), jnp.float32),
            pltpu.VMEM((seqs, joint, tokens), jnp.float32),
            dma,
            dma((5,)),
            dma((AHEAD,)),
            dma((2,)),
            dma((pj_count // CORES, chunks)),
            dma((pj_count // CORES,)),
            dma,
            dma((pj_count // CORES,)),
            dma((pj_count // CORES, 2)),
            dma,
            dma,
            dma((pi_count, 2)),
            dma,
            dma((pi_count // 2,)),
            dma((pi_count // 2,)),
            pltpu.SemaphoreType.REGULAR((pj_count // CORES - 1,)),
        ],
        compiler_params=pltpu.CompilerParams(
            collective_id=0, has_side_effects=True, vmem_limit_bytes=VMEM_LIMIT
        ),
        name="layer",
    )(
        duo,
        duo_w.T,
        aligned,
        gain[None, :],
        shift[None, :],
        payload_w,
        switch_w,
        closing_w.T,
    )


def solution(mesh):
    return jax.shard_map(
        functools.partial(body, mesh.shape["pi"], mesh.shape["pj"]),
        mesh=mesh,
        in_specs=(P("pi", "pj", None), P(), P("pj", None, "pi"), P(), P(), P(), P(), P()),
        out_specs=P("pj", None, "pi"),
        check_vma=False,
    )
```

```python
import functools

import jax
import jax.numpy as jnp
from jax import lax
from jax.experimental import pallas as pl
from jax.experimental.pallas import tpu as pltpu
from jax.sharding import PartitionSpec as P

EPS = 1e-05
MESH = pl.DeviceIdType.MESH
NT = (((1,), (1,)), ((), ()))
CORES = 2
TILE = 16
PIECE = 32
CHUNK = 32
GROUP = 16
AHEAD = 3
SLOTS = 4
SOON = 5
HELD = 3
VMEM_LIMIT = 61 << 20


def dot(a, b, dims=(((1,), (0,)), ((), ()))):
    return lax.dot_general(a, b, dims, preferred_element_type=jnp.float32)


def split_weights(w):
    w = w - jnp.mean(w, axis=1, keepdims=True)
    hi = w.astype(jnp.bfloat16).astype(jnp.float32)
    mid = (w - hi).astype(jnp.bfloat16).astype(jnp.float32)
    w3 = jnp.concatenate([hi, mid, w - hi - mid, jnp.zeros_like(w)], axis=0)
    return w3.astype(jnp.bfloat16)


def tile_scores(x, w3, centring):
    rows, cols, chans = x.shape
    heads = w3.shape[0] // 4
    x = x.reshape(rows * cols, chans)
    half = rows * cols // 2
    centred = dot(jnp.concatenate([x[:half], x[half:]], axis=1), centring)
    square = centred * centred
    one, two = square[:, :chans], square[:, chans:]
    low = lax.broadcasted_iota(jnp.int32, one.shape, 1) < chans // 2
    both = jnp.where(low, one, two) + pltpu.roll(jnp.where(low, two, one), chans // 2, 1)
    top = both.astype(jnp.bfloat16)
    rest = (both - top.astype(jnp.float32)).astype(jnp.bfloat16)
    group = lax.broadcasted_iota(jnp.int32, (2 * heads, 2 * chans), 0) // heads
    owner = lax.broadcasted_iota(jnp.int32, (2 * heads, 2 * chans), 1) % chans // (chans // 2)
    picks = jnp.where(group == owner, 1.0, 0.0).astype(jnp.bfloat16)
    sums = dot(picks, jnp.concatenate([top, rest], axis=1), NT)
    sums = [sums[g * heads : (g + 1) * heads] for g in range(2)]
    variance = jnp.concatenate(sums, axis=1) * (1.0 / chans)
    parts = dot(w3, x, NT)
    scores = parts[:heads] + (parts[heads : 2 * heads] + parts[2 * heads : 3 * heads])
    return scores * lax.rsqrt(variance + EPS)


def kernel(
    pi_count,
    pj_count,
    pair_hbm,
    w_hbm,
    msa_hbm,
    gain_hbm,
    shift_hbm,
    payload_hbm,
    switch_hbm,
    wc_hbm,
    out_ref,
    w_ref,
    gain_ref,
    shift_ref,
    payload_ref,
    switch_ref,
    wc_ref,
    wv_ref,
    ws_ref,
    spread,
    centring,
    pair,
    msa,
    ex,
    hold,
    peaks,
    turned,
    vals,
    weights,
    acc,
    gate,
    w_sem,
    small_sem,
    pair_sem,
    msa_sem,
    ex_rs,
    ex_fw,
    ex_dn,
    ex_pt,
    ex_far,
    pk_rs,
    pk_ss,
    pk_ms,
    pk_mr,
    ms_rs,
    ms_sx,
    ms_up,
    ms_dn,
    rounds,
):
    me_i, me_j = lax.axis_index("pi"), lax.axis_index("pj")
    line, yline = pj_count // CORES, pi_count // 2
    z, core = me_j // CORES, me_j % CORES
    y, x = me_i // 2, me_i % 2
    chunks = ex.shape[1]
    heads, cols = ex.shape[2], ex.shape[4]
    rows = chunks * CHUNK
    share = CHUNK // PIECE
    seqs, half, chans = out_ref.shape[0], msa.shape[1], msa.shape[2]
    span = vals.shape[2] - 16
    width = span // seqs
    mate = me_j - core + (1 - core)
    x_near = me_i - x + (1 - x)

    pair_in = lambda q: pltpu.make_async_copy(
        pair_hbm.at[pl.ds(q * PIECE, PIECE)], pair.at[q % AHEAD], pair_sem.at[q % AHEAD]
    )
    own_in = [
        pltpu.make_async_copy(msa_hbm.at[pl.ds(h * half, half)], msa.at[me_i * 2 + h], msa_sem.at[h])
        for h in range(2)
    ]
    w_in = pltpu.make_async_copy(w_hbm, w_ref, w_sem)
    w_in.start()
    for h in range(2):
        own_in[h].start()
    lax.fori_loop(0, AHEAD, lambda q, c: (pair_in(q).start(), c)[1], 0)
    small_in = [
        pltpu.make_async_copy(source, target, small_sem.at[k])
        for k, (source, target) in enumerate(
            (
                (gain_hbm, gain_ref),
                (shift_hbm, shift_ref),
                (payload_hbm, payload_ref),
                (switch_hbm, switch_ref),
                (wc_hbm, wc_ref),
            )
        )
    ]
    for copy in small_in:
        copy.start()

    barrier = pltpu.get_barrier_semaphore()

    def greet(i, j):
        pl.semaphore_signal(barrier, inc=1, device_id=(i, j), device_id_type=MESH)

    up_y, down_y = y < yline - 1, y > 0
    up_z, down_z = z < line - 1, z > 0
    near_z = 1 + jnp.where(up_z, 1, 0) + jnp.where(down_z, 1, 0)
    near_y = jnp.where(up_y, 1, 0) + jnp.where(down_y, 1, 0)

    def tell_line(tell):
        tell(me_i, mate)
        pl.when(up_z)(lambda: tell(me_i, me_j + CORES))
        pl.when(down_z)(lambda: tell(me_i, me_j - CORES))

    tell_line(greet)
    greet(x_near, me_j)
    pl.when(up_y)(lambda: greet(me_i + 2, me_j))
    pl.when(down_y)(lambda: greet(me_i - 2, me_j))

    pl.semaphore_wait(barrier, 1 + near_y + near_z)

    def msa_copy(p, h, send, i, count=1):
        part = msa.at[pl.ds(p * 2 + h, count)]
        return pltpu.make_async_remote_copy(
            part, part, send, ms_rs.at[p, h], device_id=(i, me_j), device_id_type=MESH
        )

    def to_x(p, h):
        return msa_copy(p, h, ms_sx, x_near)

    def to_up(p, h, e):
        return msa_copy(p, h, ms_up.at[e], me_i + 2)

    def to_down(p, h, e):
        return msa_copy(p, h, ms_dn.at[e], me_i - 2)

    def along_y(p, h):
        pl.when(up_y)(lambda: to_up(p, h, 0).start())
        pl.when(down_y)(lambda: to_down(p, h, 0).start())

    def take(p, h):
        to_x(p, h).wait_recv()

    for h in range(2):
        own_in[h].wait()
    to_x(me_i, 0).start()
    along_y(me_i, 1)
    to_x(me_i, 1).start()
    along_y(me_i, 0)

    def pass_y(e, column, h, cross):
        below, above = me_i - x + column - 2 * e, me_i - x + column + 2 * e

        @pl.when(y - e >= 0)
        def _():
            take(below, h)
            pl.when(up_y)(lambda: to_up(below, h, e).start())
            if cross:
                to_x(below, h).start()

        @pl.when(y + e < yline)
        def _():
            take(above, h)
            pl.when(down_y)(lambda: to_down(above, h, e).start())
            if cross:
                to_x(above, h).start()

    def first_relays():
        take(x_near, 0)
        along_y(x_near, 0)
        for e in range(1, yline):
            pass_y(e, x, 1, True)

    def ex_copy(o, q, send, receive, j):
        block = ex.at[o] if q is None else ex.at[o, q]
        return pltpu.make_async_remote_copy(
            block, block, send, receive, device_id=(me_i, j), device_id_type=MESH
        )

    def ex_along(o, q, send, j):
        c = o // CORES
        return ex_copy(o, q, send, ex_rs.at[c, 0 if q is None else q], j)

    def ex_up(o, q=None):
        return ex_along(o, q, ex_fw.at[o // CORES], me_j + CORES)

    def ex_down(o, q=None):
        return ex_along(o, q, ex_fw.at[o // CORES], me_j - CORES)

    def ex_own_down(q=None):
        return ex_along(me_j, q, ex_dn, me_j - CORES)

    def ex_mate(o, q=None):
        late = 0 if q is None else jnp.where(q >= chunks - HELD, 1, 0)
        return ex_copy(o, q, ex_pt.at[o // CORES], ex_far.at[o // CORES, late], mate)

    def ex_mate_part(o, late):
        block = ex.at[o, pl.ds(chunks - HELD, HELD) if late else pl.ds(0, chunks - HELD)]
        c = o // CORES
        return pltpu.make_async_remote_copy(
            block, block, ex_pt.at[c], ex_far.at[c, late], device_id=(me_i, mate), device_id_type=MESH
        )

    def send_own(q):
        pl.when(up_z)(lambda: ex_up(me_j, q).start())
        pl.when(down_z)(lambda: ex_own_down(q).start())
        ex_mate(me_j, q).start()

    def relay(d, q):
        below, above = me_j - CORES * d, me_j + CORES * d

        @pl.when(z - d >= 0)
        def _():
            ex_up(below, q).wait_recv()
            pl.when(up_z)(lambda: ex_up(below, q).start())
            ex_mate(below, q).start()

        @pl.when(z + d < line)
        def _():
            ex_up(above, q).wait_recv()
            pl.when(down_z)(lambda: ex_down(above, q).start())
            ex_mate(above, q).start()

    def peak_copy(block, send, receive, j):
        return pltpu.make_async_remote_copy(
            block, block, send, receive, device_id=(me_i, j), device_id_type=MESH
        )

    def own_peaks(r):
        return peak_copy(peaks.at[core, z], pk_ss, pk_rs, (me_j + CORES * r) % pj_count)

    def line_peaks():
        return peak_copy(peaks.at[core, pl.ds(0, line - 1)], pk_ss, pk_rs, mate)

    def mate_peaks():
        return peak_copy(peaks.at[core], pk_ms, pk_mr, mate)

    def tell_round(r):
        def tell(i, j):
            pl.semaphore_signal(rounds.at[r], inc=1, device_id=(i, j), device_id_type=MESH)

        tell_line(tell)

    def hear_round(r):
        pl.semaphore_wait(rounds.at[r], near_z)

    tell_round(0)
    w_in.wait()
    w3 = split_weights(w_ref[...])
    pair_chans = w3.shape[1]
    across = lax.broadcasted_iota(jnp.int32, centring.shape, 0)
    along = lax.broadcasted_iota(jnp.int32, centring.shape, 1)
    away = jnp.where(across // pair_chans == along // pair_chans, -1.0 / pair_chans, 0.0)
    centring[...] = jnp.where(across == along, 1.0 + away, away).astype(jnp.bfloat16)
    lane = lax.broadcasted_iota(jnp.int32, (heads, rows), 1)
    peaks[core, z] = jnp.zeros((heads, rows), jnp.float32)

    def pair_piece(q):
        pair_in(q).wait()
        top = peaks[core, z]
        for t in range(PIECE // TILE):
            scores = tile_scores(pair[q % AHEAD, t * TILE : (t + 1) * TILE], w3, centring[...])
            for k in range(TILE):
                one = scores[:, k * cols : (k + 1) * cols]
                peak = jnp.max(one, axis=1, keepdims=True)
                hold[:, t * TILE + k, :] = jnp.exp(one - peak)
                top = jnp.where(lane == q * PIECE + t * TILE + k, peak, top)
        peaks[core, z] = top
        at = pl.ds(pl.multiple_of(q % share * PIECE, PIECE), PIECE)
        ex[me_j, q // share, :, at, :] = hold[...].astype(jnp.bfloat16)
        pl.when(q + AHEAD < chunks * share)(lambda: pair_in(q + AHEAD).start())

    soon = min(line - 1, (chunks * share - 2) // 2)

    def next_round(r):
        hear_round(r)
        pl.when(r < line - 2)(lambda: tell_round(r + 1))

    def pair_step(q, carry):
        pair_piece(q)
        pl.when(q % share == share - 1)(lambda: send_own(q // share))

        pl.when((q >= SOON) & (q % 2 == 1))(lambda: relay(1, (q - SOON) // 2))

        @pl.when((q % 2 == 1) & (q >= 3) & (q < 3 + 2 * soon))
        def _():
            next_round((q - 3) // 2)

        return carry

    lax.fori_loop(0, chunks * share, pair_step, 0)
    lax.fori_loop(soon, line - 1, lambda r, c: (next_round(r), c)[1], 0)
    lax.fori_loop(1, line, lambda r, c: (own_peaks(r).start(), c)[1], 0)

    def relays(d, first, last):
        lax.fori_loop(first, last, lambda q, c: (relay(d, q), c)[1], 0)

    def normed(p, s):
        v = msa[p * 2 + s // half, s % half].astype(jnp.float32)
        v = v - jnp.mean(v, axis=0, keepdims=True)
        variance = jnp.mean(v * v, axis=0, keepdims=True)
        return (v * lax.rsqrt(variance + EPS) * spread[0] + spread[1]).astype(jnp.bfloat16)

    def gate_group(g, carry):
        for k in range(GROUP):
            s = g * GROUP + k
            gate[s] = jax.nn.sigmoid(dot(ws_ref[...], normed(me_i, s)))
        return carry

    for copy in small_in:
        copy.wait()
    wv_ref[...] = payload_ref[...].astype(jnp.float32).T.astype(jnp.bfloat16)
    ws_ref[...] = switch_ref[...].astype(jnp.float32).T.astype(jnp.bfloat16)
    diagonal = lax.broadcasted_iota(jnp.int32, (chans, chans), 0)
    diagonal = diagonal == lax.broadcasted_iota(jnp.int32, (chans, chans), 1)
    for k, ref in enumerate((gain_ref, shift_ref)):
        column = jnp.sum(jnp.where(diagonal, ref[...], 0.0), axis=1, keepdims=True)
        spread[k] = jnp.broadcast_to(column, (chans, rows))

    relays(1, (chunks - SOON + 1) // 2, chunks - 2)
    lax.fori_loop(0, seqs // GROUP, gate_group, 0)
    relays(1, chunks - 2, chunks)
    first_relays()

    for slot in range(SLOTS):
        vals[slot, :, span:, :] = jnp.ones((heads, 16, rows), jnp.bfloat16)

    def zero_head(h, carry):
        acc[h] = jnp.zeros(acc.shape[1:], jnp.float32)
        return carry

    lax.fori_loop(0, heads, zero_head, 0)

    def values(p, h, slot):
        def value_group(g, carry):
            for k in range(GROUP):
                s = g * GROUP + k
                v = dot(wv_ref[...], normed(p, s)).astype(jnp.bfloat16)
                at = pl.ds(pl.multiple_of(s * width, width), width)
                for n in range(heads):
                    vals[slot, n, at, :] = v[n * width : (n + 1) * width]
            return carry

        steps = half // GROUP
        lax.fori_loop(h * steps, (h + 1) * steps, value_group, 0)

    y_near = (y + 1) % yline * 2 + x

    def slot_of(p):
        return jnp.where(p == me_i, 0, jnp.where(p == x_near, 1, jnp.where(p == y_near, 2, 3)))

    def early_values(k, carry):
        p = jnp.where(k < 2, me_i, jnp.where(k == 2, x_near, y_near))
        h = jnp.where((k == 1) | (k == 3), 1, 0)
        values(p, h, slot_of(p))
        return carry

    lax.fori_loop(0, 2, early_values, 0)
    line_peaks().wait_recv()
    mate_peaks().start()
    lax.fori_loop(2, 4, early_values, 0)

    mate_peaks().wait_recv()
    top = jnp.max(peaks[...].reshape(pj_count, heads, rows), axis=0)

    def turn(o, carry):
        pad = jnp.zeros((128 - heads, rows), jnp.float32)
        turned[o] = jnp.concatenate([jnp.exp(peaks[o % CORES, o // CORES] - top), pad], axis=0).T
        return carry

    lax.fori_loop(0, pj_count, turn, 0)

    def rescale(p, slot, late):
        first, last = (chunks - HELD, chunks) if late else (0, chunks - HELD)
        ex_mate_part(p * CORES + (1 - core), late).wait_recv()
        span_rows = slice(first * CHUNK, last * CHUNK)
        for c in range(CORES):
            o = p * CORES + c
            for h in range(heads):
                e = ex[o, first:last, h].reshape((last - first) * CHUNK, cols).astype(jnp.float32)
                e = (e * turned[o, span_rows, h : h + 1]).astype(jnp.bfloat16)
                weights[slot, h, span_rows, c * cols : (c + 1) * cols] = e

    def attend(slot, weight_slot):
        for h in range(heads):
            acc[h] += dot(vals[slot, h], weights[weight_slot, h], NT)

    def apart(p):
        return jnp.where(p > z, p - z, z - p)

    def crosses(p):
        return (p // 2 != y) & (p % 2 != x)

    def farthest_from_here(p):
        return apart(p) == line - 1

    def attend_unit(p):
        near = jnp.where(apart(p) <= 1, jnp.where(p == me_i, 0, 1), apart(p))
        return jnp.where(crosses(p) | farthest_from_here(p), -1, near)

    def value_unit(p):
        beside = (p == x_near) | (p == y_near)
        return jnp.where(p == me_i, -1, jnp.where(beside, 1, attend_unit(p)))

    def late_values(p):
        pl.when(p % 2 != x)(lambda: take(p, 1))
        first = jnp.where(p == x_near, 1, 0)
        end = jnp.where(p == y_near, 1, 2)
        lax.fori_loop(first, end, lambda h, c: (values(p, h, slot_of(p)), c)[1], 0)

    half_way = chunks // 2
    diagonal_block = (y + 1) % yline * 2 + (1 - x)

    def step(n, carry):
        u, p = n // pi_count, n % pi_count
        fresh = p == 0

        @pl.when(fresh & (u == 1))
        def _():
            relays(2, 0, half_way)
            for e in range(1, yline):
                pass_y(e, x, 0, False)

        @pl.when((u == 1) & (p < chunks - half_way))
        def _():
            relay(2, half_way + p)

        @pl.when(fresh & (u >= 3))
        def _():
            relays(u, 0, chunks)

        pl.when(value_unit(p) == u)(lambda: late_values(p))

        @pl.when(attend_unit(p) == u)
        def _():
            rescale(p, 0, 0)
            rescale(p, 0, 1)
            attend(slot_of(p), 0)

        return carry

    lax.fori_loop(0, (line - 1) * pi_count, step, 0)

    at_end = (z == 0) | (z == line - 1)
    farthest = jnp.where(z == 0, line - 1, 0)

    @pl.when(jnp.logical_not(farthest_from_here(diagonal_block)))
    def _():
        rescale(diagonal_block, 2, 0)
        rescale(diagonal_block, 2, 1)

    relays(line - 1, 0, chunks - HELD)
    for e in range(1, yline):
        pass_y(e, 1 - x, 0, False)
    for e in range(1, yline):
        p = (y + e) % yline * 2 + (1 - x)
        here = jnp.logical_not(farthest_from_here(p))
        if pi_count <= SLOTS:
            late_values(p)
        else:
            pl.when(here)(lambda: late_values(p))
        if e == 1:
            relays(line - 1, chunks - HELD, chunks - 1)
            pl.when(at_end)(lambda: rescale(farthest, 1, 0))
            relay(line - 1, chunks - 1)

        @pl.when(here)
        def _():
            if e > 1:
                rescale(p, 0, 0)
                rescale(p, 0, 1)
            attend(slot_of(p), 2 if e == 1 else 0)

    @pl.when(at_end)
    def _():
        if pi_count > SLOTS:
            pl.when(slot_of(farthest) == 3)(lambda: late_values(farthest))
        rescale(farthest, 1, 1)
        attend(slot_of(farthest), 1)

    inverse = 1.0 / acc[:, span : span + 8, :]
    inverse = inverse[:, :1, :]

    def close_group(g, carry):
        for k in range(GROUP):
            s = g * GROUP + k
            at = pl.ds(pl.multiple_of(s * width, width), width)
            opened = gate[s].reshape(heads, width, rows)
            mixed = (opened * (acc[:, at, :] * inverse)).astype(jnp.bfloat16)
            out_ref[s] = dot(wc_ref[...], mixed.reshape(heads * width, rows)).astype(jnp.bfloat16)
        return carry

    lax.fori_loop(0, seqs // GROUP, close_group, 0)

    line_peaks().wait_send()
    mate_peaks().wait_send()
    msa_copy(0, 0, ms_sx, x_near, yline + 1).wait_send()
    for e in range(yline):
        pl.when(up_y & (y - e >= 0))(
            lambda: msa_copy(0, 0, ms_up.at[e], me_i + 2, 3).wait_send()
        )
        pl.when(down_y & (y + e < yline))(
            lambda: msa_copy(0, 0, ms_dn.at[e], me_i - 2, 3).wait_send()
        )
    pl.when(down_z)(lambda: ex_own_down().wait_send())

    def drain(c, carry):
        o = c * CORES + core
        ex_mate(o).wait_send()
        pl.when((c <= z) & up_z)(lambda: ex_up(o).wait_send())
        pl.when((c > z) & down_z)(lambda: ex_down(o).wait_send())
        return carry

    lax.fori_loop(0, line, drain, 0)


def body(pi_count, pj_count, duo, duo_w, aligned, gain, shift, payload_w, switch_w, closing_w):
    rows, cols, pair_chans = duo.shape
    seqs, chans, tokens = aligned.shape
    heads, joint = duo_w.shape[1], payload_w.shape[1]
    span = seqs * (joint // heads)
    chunks = rows // CHUNK
    assert tokens == rows == CORES * cols and pj_count == CORES * pi_count
    assert pi_count >= 4 and pi_count >= chunks // 2
    vmem = pl.BlockSpec(memory_space=pltpu.VMEM)
    hbm = pl.BlockSpec(memory_space=pltpu.HBM)
    dma = pltpu.SemaphoreType.DMA
    return pl.pallas_call(
        functools.partial(kernel, pi_count, pj_count),
        in_specs=[hbm] * 8,
        out_specs=vmem,
        out_shape=pltpu.VMEM(aligned.shape, jnp.bfloat16),
        scratch_shapes=[
            pltpu.VMEM((heads, pair_chans), jnp.float32),
            pltpu.VMEM((1, chans), jnp.float32),
            pltpu.VMEM((1, chans), jnp.float32),
            pltpu.VMEM(payload_w.shape, jnp.bfloat16),
            pltpu.VMEM(switch_w.shape, jnp.bfloat16),
            pltpu.VMEM(closing_w.shape[::-1], jnp.bfloat16),
            pltpu.VMEM((joint, chans), jnp.bfloat16),
            pltpu.VMEM((joint, chans), jnp.bfloat16),
            pltpu.VMEM((2, chans, rows), jnp.float32),
            pltpu.VMEM((2 * pair_chans, 2 * pair_chans), jnp.bfloat16),
            pltpu.VMEM((AHEAD, PIECE, cols, pair_chans), jnp.bfloat16),
            pltpu.VMEM((pi_count * 2, seqs // 2, chans, tokens), jnp.bfloat16),
            pltpu.VMEM((pj_count, chunks, heads, CHUNK, cols), jnp.bfloat16),
            pltpu.VMEM((heads, PIECE, cols), jnp.float32),
            pltpu.VMEM((CORES, pj_count // CORES, heads, rows), jnp.float32),
            pltpu.VMEM((pj_count, rows, 128), jnp.float32),
            pltpu.VMEM((SLOTS, heads, span + 16, rows), jnp.bfloat16),
            pltpu.VMEM((3, heads, rows, CORES * cols), jnp.bfloat16),
            pltpu.VMEM((heads, span + 16, rows), jnp.float32),
            pltpu.VMEM((seqs, joint, tokens), jnp.float32),
            dma,
            dma((5,)),
            dma((AHEAD,)),
            dma((2,)),
            dma((pj_count // CORES, chunks)),
            dma((pj_count // CORES,)),
            dma,
            dma((pj_count // CORES,)),
            dma((pj_count // CORES, 2)),
            dma,
            dma,
            dma,
            dma,
            dma((pi_count, 2)),
            dma,
            dma((pi_count // 2,)),
            dma((pi_count // 2,)),
            pltpu.SemaphoreType.REGULAR((pj_count // CORES - 1,)),
        ],
        compiler_params=pltpu.CompilerParams(
            collective_id=0, has_side_effects=True, vmem_limit_bytes=VMEM_LIMIT
        ),
        name="layer",
    )(
        duo,
        duo_w.T,
        aligned,
        gain[None, :],
        shift[None, :],
        payload_w,
        switch_w,
        closing_w.T,
    )


def solution(mesh):
    return jax.shard_map(
        functools.partial(body, mesh.shape["pi"], mesh.shape["pj"]),
        mesh=mesh,
        in_specs=(P("pi", "pj", None), P(), P("pj", None, "pi"), P(), P(), P(), P(), P()),
        out_specs=P("pj", None, "pi"),
        check_vma=False,
    )
```

```python
import functools

import jax
import jax.numpy as jnp
from jax import lax
from jax.experimental import pallas as pl
from jax.experimental.pallas import tpu as pltpu
from jax.sharding import PartitionSpec as P

EPS = 1e-05
MESH = pl.DeviceIdType.MESH
NT = (((1,), (1,)), ((), ()))
CORES = 2
TILE = 16
PIECE = 32
CHUNK = 32
GROUP = 16
AHEAD = 3
SLOTS = 4
HELD = 3
VMEM_LIMIT = 61 << 20


def dot(a, b, dims=(((1,), (0,)), ((), ()))):
    return lax.dot_general(a, b, dims, preferred_element_type=jnp.float32)


def split_weights(w):
    w = w - jnp.mean(w, axis=1, keepdims=True)
    hi = w.astype(jnp.bfloat16).astype(jnp.float32)
    mid = (w - hi).astype(jnp.bfloat16).astype(jnp.float32)
    w3 = jnp.concatenate([hi, mid, w - hi - mid, jnp.zeros_like(w)], axis=0)
    return w3.astype(jnp.bfloat16)


def tile_scores(x, w3, centring):
    rows, cols, chans = x.shape
    heads = w3.shape[0] // 4
    x = x.reshape(rows * cols, chans)
    half = rows * cols // 2
    centred = dot(jnp.concatenate([x[:half], x[half:]], axis=1), centring)
    square = centred * centred
    one, two = square[:, :chans], square[:, chans:]
    low = lax.broadcasted_iota(jnp.int32, one.shape, 1) < chans // 2
    both = jnp.where(low, one, two) + pltpu.roll(jnp.where(low, two, one), chans // 2, 1)
    top = both.astype(jnp.bfloat16)
    rest = (both - top.astype(jnp.float32)).astype(jnp.bfloat16)
    group = lax.broadcasted_iota(jnp.int32, (2 * heads, 2 * chans), 0) // heads
    owner = lax.broadcasted_iota(jnp.int32, (2 * heads, 2 * chans), 1) % chans // (chans // 2)
    picks = jnp.where(group == owner, 1.0, 0.0).astype(jnp.bfloat16)
    sums = dot(picks, jnp.concatenate([top, rest], axis=1), NT)
    sums = [sums[g * heads : (g + 1) * heads] for g in range(2)]
    variance = jnp.concatenate(sums, axis=1) * (1.0 / chans)
    parts = dot(w3, x, NT)
    scores = parts[:heads] + (parts[heads : 2 * heads] + parts[2 * heads : 3 * heads])
    return scores * lax.rsqrt(variance + EPS)


def kernel(
    pi_count,
    pj_count,
    pair_hbm,
    w_hbm,
    msa_hbm,
    gain_hbm,
    shift_hbm,
    payload_hbm,
    switch_hbm,
    wc_hbm,
    out_ref,
    w_ref,
    gain_ref,
    shift_ref,
    payload_ref,
    switch_ref,
    wc_ref,
    wv_ref,
    ws_ref,
    spread,
    centring,
    pair,
    msa,
    ex,
    hold,
    peaks,
    turned,
    vals,
    weights,
    acc,
    gate,
    w_sem,
    small_sem,
    pair_sem,
    msa_sem,
    ex_rs,
    ex_fw,
    ex_dn,
    ex_pt,
    ex_far,
    pk_rs,
    pk_ss,
    pk_ms,
    pk_mr,
    ms_rs,
    ms_sx,
    ms_up,
    ms_dn,
    rounds,
):
    me_i, me_j = lax.axis_index("pi"), lax.axis_index("pj")
    line, yline = pj_count // CORES, pi_count // 2
    z, core = me_j // CORES, me_j % CORES
    y, x = me_i // 2, me_i % 2
    chunks = ex.shape[1]
    heads, cols = ex.shape[2], ex.shape[4]
    rows = chunks * CHUNK
    share = CHUNK // PIECE
    seqs, half, chans = out_ref.shape[0], msa.shape[1], msa.shape[2]
    span = vals.shape[2] - 16
    width = span // seqs
    mate = me_j - core + (1 - core)
    x_near = me_i - x + (1 - x)

    pair_in = lambda q: pltpu.make_async_copy(
        pair_hbm.at[pl.ds(q * PIECE, PIECE)], pair.at[q % AHEAD], pair_sem.at[q % AHEAD]
    )
    own_in = [
        pltpu.make_async_copy(msa_hbm.at[pl.ds(h * half, half)], msa.at[me_i * 2 + h], msa_sem.at[h])
        for h in range(2)
    ]
    w_in = pltpu.make_async_copy(w_hbm, w_ref, w_sem)
    w_in.start()
    for h in range(2):
        own_in[h].start()
    lax.fori_loop(0, AHEAD, lambda q, c: (pair_in(q).start(), c)[1], 0)
    small_in = [
        pltpu.make_async_copy(source, target, small_sem.at[k])
        for k, (source, target) in enumerate(
            (
                (gain_hbm, gain_ref),
                (shift_hbm, shift_ref),
                (payload_hbm, payload_ref),
                (switch_hbm, switch_ref),
                (wc_hbm, wc_ref),
            )
        )
    ]
    for copy in small_in:
        copy.start()

    barrier = pltpu.get_barrier_semaphore()

    def greet(i, j):
        pl.semaphore_signal(barrier, inc=1, device_id=(i, j), device_id_type=MESH)

    up_y, down_y = y < yline - 1, y > 0
    up_z, down_z = z < line - 1, z > 0
    near_z = 1 + jnp.where(up_z, 1, 0) + jnp.where(down_z, 1, 0)
    near_y = jnp.where(up_y, 1, 0) + jnp.where(down_y, 1, 0)

    def tell_line(tell):
        tell(me_i, mate)
        pl.when(up_z)(lambda: tell(me_i, me_j + CORES))
        pl.when(down_z)(lambda: tell(me_i, me_j - CORES))

    tell_line(greet)
    greet(x_near, me_j)
    pl.when(up_y)(lambda: greet(me_i + 2, me_j))
    pl.when(down_y)(lambda: greet(me_i - 2, me_j))

    pl.semaphore_wait(barrier, 1 + near_y + near_z)

    def msa_copy(p, h, send, i, count=1):
        part = msa.at[pl.ds(p * 2 + h, count)]
        return pltpu.make_async_remote_copy(
            part, part, send, ms_rs.at[p, h], device_id=(i, me_j), device_id_type=MESH
        )

    def to_x(p, h):
        return msa_copy(p, h, ms_sx, x_near)

    def to_up(p, h, e):
        return msa_copy(p, h, ms_up.at[e], me_i + 2)

    def to_down(p, h, e):
        return msa_copy(p, h, ms_dn.at[e], me_i - 2)

    def along_y(p, h):
        pl.when(up_y)(lambda: to_up(p, h, 0).start())
        pl.when(down_y)(lambda: to_down(p, h, 0).start())

    def take(p, h):
        to_x(p, h).wait_recv()

    for h in range(2):
        own_in[h].wait()
    to_x(me_i, 0).start()
    along_y(me_i, 1)
    to_x(me_i, 1).start()
    along_y(me_i, 0)

    def pass_y(e, column, h, cross):
        below, above = me_i - x + column - 2 * e, me_i - x + column + 2 * e

        @pl.when(y - e >= 0)
        def _():
            take(below, h)
            pl.when(up_y)(lambda: to_up(below, h, e).start())
            if cross:
                to_x(below, h).start()

        @pl.when(y + e < yline)
        def _():
            take(above, h)
            pl.when(down_y)(lambda: to_down(above, h, e).start())
            if cross:
                to_x(above, h).start()

    def first_relays():
        take(x_near, 0)
        along_y(x_near, 0)
        for e in range(1, yline):
            pass_y(e, x, 1, True)

    def ex_copy(o, q, send, receive, j):
        block = ex.at[o] if q is None else ex.at[o, q]
        return pltpu.make_async_remote_copy(
            block, block, send, receive, device_id=(me_i, j), device_id_type=MESH
        )

    def ex_along(o, q, send, j):
        c = o // CORES
        return ex_copy(o, q, send, ex_rs.at[c, 0 if q is None else q], j)

    def ex_up(o, q=None):
        return ex_along(o, q, ex_fw.at[o // CORES], me_j + CORES)

    def ex_down(o, q=None):
        return ex_along(o, q, ex_fw.at[o // CORES], me_j - CORES)

    def ex_own_down(q=None):
        return ex_along(me_j, q, ex_dn, me_j - CORES)

    def ex_mate(o, q=None):
        late = 0 if q is None else jnp.where(q >= chunks - HELD, 1, 0)
        return ex_copy(o, q, ex_pt.at[o // CORES], ex_far.at[o // CORES, late], mate)

    def ex_mate_part(o, late):
        block = ex.at[o, pl.ds(chunks - HELD, HELD) if late else pl.ds(0, chunks - HELD)]
        c = o // CORES
        return pltpu.make_async_remote_copy(
            block, block, ex_pt.at[c], ex_far.at[c, late], device_id=(me_i, mate), device_id_type=MESH
        )

    def send_own(q):
        pl.when(up_z)(lambda: ex_up(me_j, q).start())
        pl.when(down_z)(lambda: ex_own_down(q).start())
        ex_mate(me_j, q).start()

    def relay(d, q):
        below, above = me_j - CORES * d, me_j + CORES * d

        @pl.when(z - d >= 0)
        def _():
            ex_up(below, q).wait_recv()
            pl.when(up_z)(lambda: ex_up(below, q).start())
            ex_mate(below, q).start()

        @pl.when(z + d < line)
        def _():
            ex_up(above, q).wait_recv()
            pl.when(down_z)(lambda: ex_down(above, q).start())
            ex_mate(above, q).start()

    def peak_copy(block, send, receive, j):
        return pltpu.make_async_remote_copy(
            block, block, send, receive, device_id=(me_i, j), device_id_type=MESH
        )

    def own_peaks(r):
        return peak_copy(peaks.at[core, z], pk_ss, pk_rs, (me_j + CORES * r) % pj_count)

    def line_peaks():
        return peak_copy(peaks.at[core, pl.ds(0, line - 1)], pk_ss, pk_rs, mate)

    def mate_peaks():
        return peak_copy(peaks.at[core], pk_ms, pk_mr, mate)

    def tell_round(r):
        def tell(i, j):
            pl.semaphore_signal(rounds.at[r], inc=1, device_id=(i, j), device_id_type=MESH)

        tell_line(tell)

    def hear_round(r):
        pl.semaphore_wait(rounds.at[r], near_z)

    tell_round(0)
    w_in.wait()
    w3 = split_weights(w_ref[...])
    pair_chans = w3.shape[1]
    across = lax.broadcasted_iota(jnp.int32, centring.shape, 0)
    along = lax.broadcasted_iota(jnp.int32, centring.shape, 1)
    away = jnp.where(across // pair_chans == along // pair_chans, -1.0 / pair_chans, 0.0)
    centring[...] = jnp.where(across == along, 1.0 + away, away).astype(jnp.bfloat16)
    lane = lax.broadcasted_iota(jnp.int32, (heads, rows), 1)
    peaks[core, z] = jnp.zeros((heads, rows), jnp.float32)

    def pair_piece(q):
        pair_in(q).wait()
        top = peaks[core, z]
        for t in range(PIECE // TILE):
            scores = tile_scores(pair[q % AHEAD, t * TILE : (t + 1) * TILE], w3, centring[...])
            for k in range(TILE):
                one = scores[:, k * cols : (k + 1) * cols]
                peak = jnp.max(one, axis=1, keepdims=True)
                hold[:, t * TILE + k, :] = jnp.exp(one - peak)
                top = jnp.where(lane == q * PIECE + t * TILE + k, peak, top)
        peaks[core, z] = top
        at = pl.ds(pl.multiple_of(q % share * PIECE, PIECE), PIECE)
        ex[me_j, q // share, :, at, :] = hold[...].astype(jnp.bfloat16)
        pl.when(q + AHEAD < chunks * share)(lambda: pair_in(q + AHEAD).start())

    soon = min(line - 1, (chunks * share - 2) // 2)

    def next_round(r):
        hear_round(r)
        pl.when(r < line - 2)(lambda: tell_round(r + 1))

    def pair_step(q, carry):
        pair_piece(q)
        pl.when(q % share == share - 1)(lambda: send_own(q // share))

        @pl.when((q % 2 == 1) & (q >= 3) & (q < 3 + 2 * soon))
        def _():
            next_round((q - 3) // 2)

        return carry

    lax.fori_loop(0, chunks * share, pair_step, 0)
    lax.fori_loop(soon, line - 1, lambda r, c: (next_round(r), c)[1], 0)
    lax.fori_loop(1, line, lambda r, c: (own_peaks(r).start(), c)[1], 0)

    def relays(d, first, last):
        lax.fori_loop(first, last, lambda q, c: (relay(d, q), c)[1], 0)

    def normed(p, s):
        v = msa[p * 2 + s // half, s % half].astype(jnp.float32)
        v = v - jnp.mean(v, axis=0, keepdims=True)
        variance = jnp.mean(v * v, axis=0, keepdims=True)
        return (v * lax.rsqrt(variance + EPS) * spread[0] + spread[1]).astype(jnp.bfloat16)

    def gate_group(g, carry):
        for k in range(GROUP):
            s = g * GROUP + k
            gate[s] = jax.nn.sigmoid(dot(ws_ref[...], normed(me_i, s)))
        return carry

    for copy in small_in:
        copy.wait()
    wv_ref[...] = payload_ref[...].astype(jnp.float32).T.astype(jnp.bfloat16)
    ws_ref[...] = switch_ref[...].astype(jnp.float32).T.astype(jnp.bfloat16)
    diagonal = lax.broadcasted_iota(jnp.int32, (chans, chans), 0)
    diagonal = diagonal == lax.broadcasted_iota(jnp.int32, (chans, chans), 1)
    for k, ref in enumerate((gain_ref, shift_ref)):
        column = jnp.sum(jnp.where(diagonal, ref[...], 0.0), axis=1, keepdims=True)
        spread[k] = jnp.broadcast_to(column, (chans, rows))

    relays(1, 0, chunks - 2)
    lax.fori_loop(0, seqs // GROUP, gate_group, 0)
    relays(1, chunks - 2, chunks)
    first_relays()

    for slot in range(SLOTS):
        vals[slot, :, span:, :] = jnp.ones((heads, 16, rows), jnp.bfloat16)

    def zero_head(h, carry):
        acc[h] = jnp.zeros(acc.shape[1:], jnp.float32)
        return carry

    lax.fori_loop(0, heads, zero_head, 0)

    def values(p, h, slot):
        def value_group(g, carry):
            for k in range(GROUP):
                s = g * GROUP + k
                v = dot(wv_ref[...], normed(p, s)).astype(jnp.bfloat16)
                at = pl.ds(pl.multiple_of(s * width, width), width)
                for n in range(heads):
                    vals[slot, n, at, :] = v[n * width : (n + 1) * width]
            return carry

        steps = half // GROUP
        lax.fori_loop(h * steps, (h + 1) * steps, value_group, 0)

    y_near = (y + 1) % yline * 2 + x

    def slot_of(p):
        return jnp.where(p == me_i, 0, jnp.where(p == x_near, 1, jnp.where(p == y_near, 2, 3)))

    def early_values(k, carry):
        p = jnp.where(k < 2, me_i, jnp.where(k == 2, x_near, y_near))
        h = jnp.where((k == 1) | (k == 3), 1, 0)
        values(p, h, slot_of(p))
        return carry

    lax.fori_loop(0, 2, early_values, 0)
    line_peaks().wait_recv()
    mate_peaks().start()
    lax.fori_loop(2, 4, early_values, 0)

    mate_peaks().wait_recv()
    top = jnp.max(peaks[...].reshape(pj_count, heads, rows), axis=0)

    def turn(o, carry):
        pad = jnp.zeros((128 - heads, rows), jnp.float32)
        turned[o] = jnp.concatenate([jnp.exp(peaks[o % CORES, o // CORES] - top), pad], axis=0).T
        return carry

    lax.fori_loop(0, pj_count, turn, 0)

    def rescale(p, slot, late):
        first, last = (chunks - HELD, chunks) if late else (0, chunks - HELD)
        ex_mate_part(p * CORES + (1 - core), late).wait_recv()
        span_rows = slice(first * CHUNK, last * CHUNK)
        for c in range(CORES):
            o = p * CORES + c
            for h in range(heads):
                e = ex[o, first:last, h].reshape((last - first) * CHUNK, cols).astype(jnp.float32)
                e = (e * turned[o, span_rows, h : h + 1]).astype(jnp.bfloat16)
                weights[slot, h, span_rows, c * cols : (c + 1) * cols] = e

    def attend(slot, weight_slot):
        for h in range(heads):
            acc[h] += dot(vals[slot, h], weights[weight_slot, h], NT)

    def apart(p):
        return jnp.where(p > z, p - z, z - p)

    def crosses(p):
        return (p // 2 != y) & (p % 2 != x)

    def farthest_from_here(p):
        return apart(p) == line - 1

    def attend_unit(p):
        near = jnp.where(apart(p) <= 1, jnp.where(p == me_i, 0, 1), apart(p))
        return jnp.where(crosses(p) | farthest_from_here(p), -1, near)

    def value_unit(p):
        beside = (p == x_near) | (p == y_near)
        return jnp.where(p == me_i, -1, jnp.where(beside, 1, attend_unit(p)))

    def late_values(p):
        pl.when(p % 2 != x)(lambda: take(p, 1))
        first = jnp.where(p == x_near, 1, 0)
        end = jnp.where(p == y_near, 1, 2)
        lax.fori_loop(first, end, lambda h, c: (values(p, h, slot_of(p)), c)[1], 0)

    half_way = chunks // 2
    diagonal_block = (y + 1) % yline * 2 + (1 - x)

    def step(n, carry):
        u, p = n // pi_count, n % pi_count
        fresh = p == 0

        @pl.when(fresh & (u == 1))
        def _():
            relays(2, 0, half_way)
            for e in range(1, yline):
                pass_y(e, x, 0, False)

        @pl.when((u == 1) & (p < chunks - half_way))
        def _():
            relay(2, half_way + p)

        @pl.when(fresh & (u >= 3))
        def _():
            relays(u, 0, chunks)

        pl.when(value_unit(p) == u)(lambda: late_values(p))

        @pl.when(attend_unit(p) == u)
        def _():
            rescale(p, 0, 0)
            rescale(p, 0, 1)
            attend(slot_of(p), 0)

        return carry

    lax.fori_loop(0, (line - 1) * pi_count, step, 0)

    at_end = (z == 0) | (z == line - 1)
    farthest = jnp.where(z == 0, line - 1, 0)

    @pl.when(jnp.logical_not(farthest_from_here(diagonal_block)))
    def _():
        rescale(diagonal_block, 2, 0)
        rescale(diagonal_block, 2, 1)

    relays(line - 1, 0, chunks - HELD)
    for e in range(1, yline):
        pass_y(e, 1 - x, 0, False)
    for e in range(1, yline):
        p = (y + e) % yline * 2 + (1 - x)
        here = jnp.logical_not(farthest_from_here(p))
        if pi_count <= SLOTS:
            late_values(p)
        else:
            pl.when(here)(lambda: late_values(p))
        if e == 1:
            relays(line - 1, chunks - HELD, chunks - 1)
            pl.when(at_end)(lambda: rescale(farthest, 1, 0))
            relay(line - 1, chunks - 1)

        @pl.when(here)
        def _():
            if e > 1:
                rescale(p, 0, 0)
                rescale(p, 0, 1)
            attend(slot_of(p), 2 if e == 1 else 0)

    @pl.when(at_end)
    def _():
        if pi_count > SLOTS:
            pl.when(slot_of(farthest) == 3)(lambda: late_values(farthest))
        rescale(farthest, 1, 1)
        attend(slot_of(farthest), 1)

    inverse = 1.0 / acc[:, span : span + 8, :]
    inverse = inverse[:, :1, :]

    def close_group(g, carry):
        for k in range(GROUP):
            s = g * GROUP + k
            at = pl.ds(pl.multiple_of(s * width, width), width)
            opened = gate[s].reshape(heads, width, rows)
            mixed = (opened * (acc[:, at, :] * inverse)).astype(jnp.bfloat16)
            out_ref[s] = dot(wc_ref[...], mixed.reshape(heads * width, rows)).astype(jnp.bfloat16)
        return carry

    lax.fori_loop(0, seqs // GROUP, close_group, 0)

    line_peaks().wait_send()
    mate_peaks().wait_send()
    msa_copy(0, 0, ms_sx, x_near, yline + 1).wait_send()
    for e in range(yline):
        pl.when(up_y & (y - e >= 0))(
            lambda: msa_copy(0, 0, ms_up.at[e], me_i + 2, 3).wait_send()
        )
        pl.when(down_y & (y + e < yline))(
            lambda: msa_copy(0, 0, ms_dn.at[e], me_i - 2, 3).wait_send()
        )
    pl.when(down_z)(lambda: ex_own_down().wait_send())

    def drain(c, carry):
        o = c * CORES + core
        ex_mate(o).wait_send()
        pl.when((c <= z) & up_z)(lambda: ex_up(o).wait_send())
        pl.when((c > z) & down_z)(lambda: ex_down(o).wait_send())
        return carry

    lax.fori_loop(0, line, drain, 0)


def body(pi_count, pj_count, duo, duo_w, aligned, gain, shift, payload_w, switch_w, closing_w):
    rows, cols, pair_chans = duo.shape
    seqs, chans, tokens = aligned.shape
    heads, joint = duo_w.shape[1], payload_w.shape[1]
    span = seqs * (joint // heads)
    chunks = rows // CHUNK
    assert tokens == rows == CORES * cols and pj_count == CORES * pi_count
    assert pi_count >= 4 and pi_count >= chunks // 2
    vmem = pl.BlockSpec(memory_space=pltpu.VMEM)
    hbm = pl.BlockSpec(memory_space=pltpu.HBM)
    dma = pltpu.SemaphoreType.DMA
    return pl.pallas_call(
        functools.partial(kernel, pi_count, pj_count),
        in_specs=[hbm] * 8,
        out_specs=vmem,
        out_shape=pltpu.VMEM(aligned.shape, jnp.bfloat16),
        scratch_shapes=[
            pltpu.VMEM((heads, pair_chans), jnp.float32),
            pltpu.VMEM((1, chans), jnp.float32),
            pltpu.VMEM((1, chans), jnp.float32),
            pltpu.VMEM(payload_w.shape, jnp.bfloat16),
            pltpu.VMEM(switch_w.shape, jnp.bfloat16),
            pltpu.VMEM(closing_w.shape[::-1], jnp.bfloat16),
            pltpu.VMEM((joint, chans), jnp.bfloat16),
            pltpu.VMEM((joint, chans), jnp.bfloat16),
            pltpu.VMEM((2, chans, rows), jnp.float32),
            pltpu.VMEM((2 * pair_chans, 2 * pair_chans), jnp.bfloat16),
            pltpu.VMEM((AHEAD, PIECE, cols, pair_chans), jnp.bfloat16),
            pltpu.VMEM((pi_count * 2, seqs // 2, chans, tokens), jnp.bfloat16),
            pltpu.VMEM((pj_count, chunks, heads, CHUNK, cols), jnp.bfloat16),
            pltpu.VMEM((heads, PIECE, cols), jnp.float32),
            pltpu.VMEM((CORES, pj_count // CORES, heads, rows), jnp.float32),
            pltpu.VMEM((pj_count, rows, 128), jnp.float32),
            pltpu.VMEM((SLOTS, heads, span + 16, rows), jnp.bfloat16),
            pltpu.VMEM((3, heads, rows, CORES * cols), jnp.bfloat16),
            pltpu.VMEM((heads, span + 16, rows), jnp.float32),
            pltpu.VMEM((seqs, joint, tokens), jnp.float32),
            dma,
            dma((5,)),
            dma((AHEAD,)),
            dma((2,)),
            dma((pj_count // CORES, chunks)),
            dma((pj_count // CORES,)),
            dma,
            dma((pj_count // CORES,)),
            dma((pj_count // CORES, 2)),
            dma,
            dma,
            dma,
            dma,
            dma((pi_count, 2)),
            dma,
            dma((pi_count // 2,)),
            dma((pi_count // 2,)),
            pltpu.SemaphoreType.REGULAR((pj_count // CORES - 1,)),
        ],
        compiler_params=pltpu.CompilerParams(
            collective_id=0, has_side_effects=True, vmem_limit_bytes=VMEM_LIMIT
        ),
        name="layer",
    )(
        duo,
        duo_w.T,
        aligned,
        gain[None, :],
        shift[None, :],
        payload_w,
        switch_w,
        closing_w.T,
    )


def solution(mesh):
    return jax.shard_map(
        functools.partial(body, mesh.shape["pi"], mesh.shape["pj"]),
        mesh=mesh,
        in_specs=(P("pi", "pj", None), P(), P("pj", None, "pi"), P(), P(), P(), P(), P()),
        out_specs=P("pj", None, "pi"),
        check_vma=False,
    )
```
